256 devices in a mesh: pp: 2 (over core), ep: 64 (over x, z_lo, y), tp: 2 (over z_hi).
Axes of the slice: x: 4, y: 4, z: 8 (z_hi: 2, z_lo: 4; z = z_hi * 4 + z_lo), core: 2. Of those that a mesh axis runs over, the one named last changes fastest.
Arguments:
- acts: bfloat16 [2, 384, 3072], P(None, 'ep'), may hold values from -6 to 6
- route_ids: int32 [2, 2, 384, 8], P('pp', None, 'ep'), may hold values from 0 to 95, all different within a row; in each aligned block of 6 rows (0 to 5, 6 to 11, ..., all dimensions but the last counted through in order) at most 2 rows name the same one
- norm_gain: bfloat16 [2, 3072], P('pp'), may hold values from 0.5 to 1.5
- router: bfloat16 [2, 3072, 96], P('pp'), may hold values from -0.109375 to 0.109375
- dense_gate: bfloat16 [2, 3072, 6144], P('pp', None, ('ep', 'tp')), may hold values from -0.109375 to 0.109375
- dense_up: bfloat16 [2, 3072, 6144], P('pp', None, ('ep', 'tp')), may hold values from -0.109375 to 0.109375
- dense_down: bfloat16 [2, 6144, 3072], P('pp', ('ep', 'tp')), may hold values from -0.078125 to 0.078125
- expert_gate: bfloat16 [2, 64, 3072, 1024], P('pp', 'ep', None, 'tp'), may hold values from -0.109375 to 0.109375
- expert_up: bfloat16 [2, 64, 3072, 1024], P('pp', 'ep', None, 'tp'), may hold values from -0.109375 to 0.109375
- expert_down: bfloat16 [2, 64, 1024, 3072], P('pp', 'ep', 'tp'), may hold values from -0.1875 to 0.1875
Outputs:
- layer_out: bfloat16 [2, 2, 384, 3072], P('pp', None, 'ep')
The draws below stay inside these ranges and needn't reach their ends.
Inputs may be any that keep to these rules, and one draw needn't show every extreme that they name: `route_ids`: the 8 ids of a token differ. In each layer and microbatch, among the 6 tokens of one ep index no id is named by more than 2 tokens, a bound that some block reaches.
All inputs are finite; a program needn't handle non-finite values.
Results may differ from the reference program's by a relative error of at most 0.008.
Values may be sent and summed in bfloat16 or wider, within the bound.
A program may use at most 128 MiB of HBM per device.

```python
import math
import jax
import jax.numpy as jnp
import numpy as np
from jax import lax

D = 3072
FFE = 1024
DFF = 6144
TOPK = 8
T_EP = 6
N_MB = 2
E = 64
E_ALL = 96
CAP = 2
MB = 384
N_EP = 64


def steps_of(own_key, extent, pieces, least, largest):
    def one(axis_at, parts):
        steps = jax.random.uniform(jax.random.fold_in(jax.random.fold_in(own_key, 6), axis_at), (parts,), jnp.float32, least / len(pieces), largest / len(pieces))
        return jnp.repeat(jnp.exp(steps), extent[axis_at] // parts).reshape((-1,) + (1,) * (len(extent) - axis_at - 1))

    factor_of = one(*pieces[0])
    for cut in pieces[1:]:
        factor_of = factor_of * one(*cut)
    return factor_of


def assign_block(rng, own, number, rows, amount, top, most, skew):
    order = jax.random.permutation(rng, amount)
    heavy_load, common = portions_of(amount, rows * top, most, skew, True), portions_of(amount, rows * top, most, skew, False)
    places = jnp.arange(amount)

    def named(sizes, rotation):
        used = int((sizes > 0).sum())
        fixed = max(1, used // 4)
        shifted = fixed + (places - fixed + rotation * (used - fixed)) % max(1, amount - fixed)
        return jnp.zeros((amount,), jnp.int32).at[order[jnp.where(places < fixed, places, shifted)]].set(jnp.asarray(sizes, jnp.int32))

    sizes = jnp.where(number % 4 == 0, named(heavy_load, number // 4), named(common, number - number // 4 - 1))
    mixed = jax.random.permutation(jax.random.fold_in(own, 3), amount)
    giver, sink = mixed[0:amount // 2 * 2:2], mixed[1:amount // 2 * 2:2]
    room = jnp.minimum(sizes[giver] - 1, most - sizes[sink]) // 2
    room = jnp.where((giver == order[0]) | (sink == order[0]) | (sizes[sink] == 0), 0, jnp.maximum(room, 0))
    shifted = jax.random.randint(jax.random.fold_in(own, 4), (amount // 2,), 0, 1 << 20) % (room + 1)
    sizes = sizes.at[giver].add(-shifted).at[sink].add(shifted)
    members = jnp.searchsorted(jnp.cumsum(sizes), jnp.arange(rows * top), side="right").astype(jnp.int32)
    table = members.reshape(top, rows).T
    table = table[jax.random.permutation(jax.random.fold_in(own, 1), rows)]
    rotation = jax.random.randint(jax.random.fold_in(own, 2), (rows, 1), 0, top)
    return jnp.take_along_axis(table, (jnp.arange(top)[None, :] + rotation) % top, axis=1)


def portions_of(amount, total, limit, lean, full):
    loads = [(1 << 20) // math.isqrt(grade ** lean) + 1 for grade in range(1, amount + 1)]
    largest = limit if full else min(limit, max(-(-total // amount), total * loads[0] // sum(loads)))
    least = 1 if total - largest >= amount - 1 else 0
    holding, rest = [largest] + [least] * (amount - 1), total - largest - least * (amount - 1)
    while rest > 0:
        candidates = [i for i in range(1, amount) if holding[i] < largest] or [i for i in range(1, amount) if holding[i] < limit]
        whole, remaining = sum([loads[i] for i in candidates]), rest
        for i in candidates:
            extra = min(limit - holding[i], max(1, remaining * loads[i] // whole), rest)
            holding[i] = holding[i] + extra
            rest = rest - extra
    return np.array(holding)


def bell_draw(key, shape, scale, limit, shards=(), kind=jnp.bfloat16):
    result = jax.random.normal(key, shape, jnp.float32) * scale
    if len(shards) > 0:
        result = steps_of(key, shape, shards, -0.22, 0.18) * result
    return jnp.clip(result, min=-limit, max=limit).astype(kind)


def setup_inputs(seed: int = 0) -> dict:
    keys = jax.random.split(jax.random.key(seed), 11)
    acts = bell_draw(keys[0], (N_MB, MB, D), 1.0, 6.0, ((1, 64),))
    route_ids_keys = jax.random.split(jax.random.fold_in(keys[1], 1), 2 * N_MB * MB // T_EP)
    route_ids_turns = jax.random.permutation(jax.random.fold_in(keys[1], 3), 2 * N_MB * MB // T_EP)
    route_ids = jax.vmap(lambda own, number: assign_block(jax.random.fold_in(keys[1], 2), own, number, T_EP, E_ALL, TOPK, CAP, 2))(route_ids_keys, route_ids_turns).reshape((2, N_MB, MB, TOPK))
    norm_gain = jnp.clip(1.0 + 0.1 * jax.random.normal(keys[2], (2, D), jnp.float32), 0.5, 1.5).astype(jnp.bfloat16)
    router = bell_draw(keys[3], (2, D, E_ALL), D ** -0.5, 0.109375, ((0, 2),))
    dense_gate = bell_draw(keys[4], (2, D, DFF), D ** -0.5, 0.109375, ((0, 2), (2, 128)))
    dense_up = bell_draw(keys[5], (2, D, DFF), D ** -0.5, 0.109375, ((0, 2), (2, 128)))
    dense_down = bell_draw(keys[6], (2, DFF, D), DFF ** -0.5, 0.078125, ((0, 2), (1, 128)))
    expert_gate = bell_draw(keys[7], (2, E, D, FFE), D ** -0.5, 0.109375, ((0, 2), (1, 64), (3, 2)))
    expert_up = bell_draw(keys[8], (2, E, D, FFE), D ** -0.5, 0.109375, ((0, 2), (1, 64), (3, 2)))
    expert_down = bell_draw(keys[9], (2, E, FFE, D), FFE ** -0.5, 0.1875, ((0, 2), (1, 64), (2, 2)))
    return {"acts": acts, "route_ids": route_ids, "norm_gain": norm_gain, "router": router, "dense_gate": dense_gate, "dense_up": dense_up, "dense_down": dense_down, "expert_gate": expert_gate, "expert_up": expert_up, "expert_down": expert_down}


def normalize(inputs, gain):
    widened = inputs.astype(jnp.float32)
    spread = lax.optimization_barrier(jnp.mean(widened * widened, axis=-1, keepdims=True))
    normed = (widened * lax.rsqrt(spread + 1e-06) * gain.astype(jnp.float32)).astype(jnp.bfloat16)
    return (widened, normed)

def gated_block(inputs, w_gate, w_up, w_down):
    gate_part = jnp.dot(inputs, w_gate, preferred_element_type=jnp.float32)
    up_part = jnp.dot(inputs, w_up, preferred_element_type=jnp.float32)
    hidden = (jax.nn.silu(gate_part) * up_part).astype(jnp.bfloat16)
    return jnp.dot(hidden, w_down, preferred_element_type=jnp.float32)

def choice_weights(normed, route_rows, router_w, n_real):
    n_total = router_w.shape[1]
    gates = jax.nn.sigmoid(jnp.dot(normed, router_w, preferred_element_type=jnp.float32))
    picked = (route_rows[:, :, None] == jnp.arange(n_total, dtype=jnp.int32)[None, None, :]).astype(jnp.float32)
    weights = lax.optimization_barrier(jnp.sum(picked * gates[:, None, :], axis=-1))
    zero_share = lax.optimization_barrier(jnp.sum(jnp.where(route_rows >= n_real, weights, jnp.float32(0.0)), axis=-1))
    return (weights, picked, zero_share)

def layer_ref(inputs, route_rows, gain, router_w, d_gate, d_up, d_down, e_gate, e_up, e_down):
    widened, normed = normalize(inputs, gain)
    n_real = e_gate.shape[0]
    weights, picked, zero_share = choice_weights(normed, route_rows, router_w, n_real)
    coef = jnp.einsum('tk,tke->te', weights, picked[:, :, :n_real], precision=lax.Precision.HIGHEST)
    dense = gated_block(normed, d_gate, d_up, d_down)
    token_count = inputs.shape[0]
    buffer_rows = min(token_count, N_EP * CAP)
    slot_range = jnp.arange(buffer_rows, dtype=jnp.float32)

    def one_expert(expert, total):
        hot = lax.optimization_barrier(jnp.sum((route_rows == expert).astype(jnp.float32), axis=-1))
        position = jnp.cumsum(hot) - hot
        select = hot[None, :] * (position[None, :] == slot_range[:, None]).astype(jnp.float32)
        chosen = jnp.dot(select.astype(jnp.bfloat16), normed, preferred_element_type=jnp.float32).astype(jnp.bfloat16)
        produced = gated_block(chosen, e_gate[expert], e_up[expert], e_down[expert])
        column = lax.dynamic_slice_in_dim(coef, expert, 1, 1)
        return total + jnp.dot(select.T, produced, precision=lax.Precision.HIGHEST) * column
    routed = lax.fori_loop(0, n_real, one_expert, jnp.zeros(widened.shape, jnp.float32))
    return (widened + dense + routed + zero_share[:, None] * normed.astype(jnp.float32)).astype(jnp.bfloat16)

def reference(acts, route_ids, norm_gain, router, dense_gate, dense_up, dense_down, expert_gate, expert_up, expert_down):
    first_section = []
    second_section = []
    for micro in range(N_MB):
        early = layer_ref(acts[micro], route_ids[0, micro], norm_gain[0], router[0], dense_gate[0], dense_up[0], dense_down[0], expert_gate[0], expert_up[0], expert_down[0])
        late = layer_ref(early, route_ids[1, micro], norm_gain[1], router[1], dense_gate[1], dense_up[1], dense_down[1], expert_gate[1], expert_up[1], expert_down[1])
        first_section.append(early)
        second_section.append(late)
    return jnp.stack([jnp.stack(first_section), jnp.stack(second_section)])
```

```python
import functools

import jax
import jax.numpy as jnp
from jax import lax
from jax.experimental import pallas as pl
from jax.experimental.pallas import tpu as pltpu
from jax.sharding import Mesh
from jax.sharding import PartitionSpec as P

MESH = pl.DeviceIdType.MESH
EP = ("ep_0", "ep_1", "ep_2")
EP_TP = ("ep_0", "ep_1", "ep_2", "tp")
F32 = jnp.float32
BF16 = jnp.bfloat16
ROWS = 8
LANES = 128


def kernel(cfg, *refs):
    (acts, routes, gain, router_h, dg_h, du_h, dd_h, eg_h, eu_h, ed_h, out) = refs[:11]
    (G, PT, R1, S1, R2, S2, R3, TS, TR, X, OB, CODE, MASK, ZS) = refs[11:25]
    (RT, DG, DU, EG, EU, ED, W1, LH, DN, CH) = refs[25:35]
    (w_sem, ag_s, ag_r, rs_s, rs_r, tp_s, tp_r, pp_s, pp_r) = refs[35:]
    sizes, n_tp, width, n_micro, n_tok, topk, n_real, n_total, slots, chunk = cfg
    n_blocks = sizes[0] * sizes[1] * sizes[2]
    rows = n_blocks * ROWS
    n_slots = n_blocks * slots
    part = width // 3
    offs = (0, part, 2 * part)
    gw = (part, part, part + LANES)
    order = ((0, 1, 2), (1, 2, 0), (2, 0, 1))

    sec = lax.axis_index("pp")
    me = tuple(lax.axis_index(a) for a in EP)
    tp = lax.axis_index("tp")
    group = (me[0] * sizes[1] + me[1]) * sizes[2] + me[2]

    def peer(axis, o):
        n = sizes[axis]
        if axis != 1:
            return {EP[axis]: lax.rem(me[axis] + o + n, n)}
        step = o if abs(o) <= n // 2 else o - n * (o // abs(o))
        z = lax.rem(tp * n + me[1] + step + n * n_tp, n * n_tp)
        return {"ep_1": lax.rem(z, n), "tp": z // n}

    far = {"tp": 1 - tp}
    above = {"pp": 1 - sec}

    def weight_copies():
        pairs = ((router_h.at[0], RT), (dg_h.at[0], DG), (du_h.at[0], DU), (dd_h.at[0], DN.at[pl.ds(0, dd_h.shape[1])]),
                 (eg_h.at[0, 0], EG), (eu_h.at[0, 0], EU), (ed_h.at[0, 0], ED))
        return [pltpu.make_async_copy(s, d, w_sem.at[i]) for i, (s, d) in enumerate(pairs)]

    for c in weight_copies():
        c.start()

    X[...] = jnp.zeros_like(X)
    barrier = pltpu.get_barrier_semaphore()
    greeted = 0
    for axis in range(3):
        for o in range(1, sizes[axis]):
            pl.semaphore_signal(barrier, inc=1, device_id=peer(axis, -o), device_id_type=MESH)
            greeted += 1
    for who in (far, above):
        pl.semaphore_signal(barrier, inc=1, device_id=who, device_id_type=MESH)
        greeted += 1

    CODE[...] = jnp.zeros_like(CODE)
    MASK[...] = jnp.zeros_like(MASK)
    W1[...] = jnp.zeros_like(W1)
    DN[pl.ds(dd_h.shape[1], LANES - dd_h.shape[1])] = jnp.zeros((LANES - dd_h.shape[1], width), BF16)
    for m in range(n_micro):
        ids = routes[0, m]
        lane = lax.broadcasted_iota(jnp.int32, (n_tok, LANES), 1)
        named = jnp.zeros((n_tok, LANES), F32)
        for k in range(topk):
            named += (ids[:, k : k + 1] == lane).astype(F32)
        MASK[m, 0:n_tok] = named
        before = jnp.zeros((1, LANES), F32)
        for t in range(n_tok):
            row = named[t : t + 1]
            CODE[m, t : t + 1] = row * (before + 1.0)
            before += row

    pl.semaphore_wait(barrier, greeted)

    def ag_copy(m, p, s, o):
        axes = order[p]
        at = [me[0], me[1], me[2]]
        for a in axes[:s]:
            at[a] = slice(None)
        ref = G.at[m, at[0], at[1], at[2], :, pl.ds(offs[p], gw[p])]
        return pltpu.make_async_remote_copy(
            src_ref=ref, dst_ref=ref, send_sem=ag_s.at[m, p, s, o - 1], recv_sem=ag_r.at[m, p, s, o - 1],
            device_id=peer(axes[s], o), device_id_type=MESH)

    def ag_start(m, p, s):
        for o in range(1, sizes[order[p][s]]):
            ag_copy(m, p, s, o).start()

    def ag_wait(m, p, s):
        for o in range(1, sizes[order[p][s]]):
            ag_copy(m, p, s, o).wait_recv()

    def rs_refs(m, p, s, o):
        axis = order[p][2 - s]
        there = lax.rem(me[axis] + o, sizes[axis])
        if s == 0:
            at = [slice(None)] * 3
            at[axis] = there
            return PT.at[m, at[0], at[1], at[2], :, pl.ds(offs[p], part)], R1.at[m, p, o - 1]
        if s == 1:
            rest = [d for d in range(3) if d != order[p][2]]
            at = [slice(None)] * 2
            at[rest.index(axis)] = there
            return S1.at[m, p, at[0], at[1]], R2.at[m, p, o - 1]
        return S2.at[m, p, there], R3.at[m, p, o - 1]

    def rs_copy(m, p, s, o):
        src, dst = rs_refs(m, p, s, o)
        return pltpu.make_async_remote_copy(
            src_ref=src, dst_ref=dst, send_sem=rs_s.at[m, p, s, o - 1], recv_sem=rs_r.at[m, p, s, o - 1],
            device_id=peer(order[p][2 - s], o), device_id_type=MESH)

    def rs_start(m, p, s):
        for o in range(1, sizes[order[p][2 - s]]):
            rs_copy(m, p, s, o).start()

    def rs_wait(m, p, s):
        for o in range(1, sizes[order[p][2 - s]]):
            rs_copy(m, p, s, o).wait_recv()

    def tp_copy(m):
        return pltpu.make_async_remote_copy(
            src_ref=TS.at[m], dst_ref=TR.at[m], send_sem=tp_s.at[m], recv_sem=tp_r.at[m],
            device_id=far, device_id_type=MESH)

    def pp_copy(m):
        return pltpu.make_async_remote_copy(
            src_ref=OB.at[m], dst_ref=X.at[m], send_sem=pp_s.at[m], recv_sem=pp_r.at[m],
            device_id=above, device_id_type=MESH)

    def take_input(m):
        @pl.when(sec == 0)
        def _():
            X[m, 0:n_tok] = acts[m]

        @pl.when(sec == 1)
        def _():
            pp_copy(m).wait_recv()

    def norm_and_send(m):
        wide = X[m].astype(F32)
        spread = jnp.mean(wide * wide, axis=-1, keepdims=True)
        normed = (wide * lax.rsqrt(spread + 1e-06) * gain[...].astype(F32)).astype(BF16)
        G[m, me[0], me[1], me[2], :, pl.ds(0, width)] = normed
        G[m, me[0], me[1], me[2], :, pl.ds(width, LANES)] = CODE[m].astype(BF16)
        for p in range(3):
            ag_start(m, p, 0)

    def zero_share(m):
        normed = G[m, me[0], me[1], me[2], :, pl.ds(0, width)]
        gates = jax.nn.sigmoid(jnp.dot(normed, RT[...], preferred_element_type=F32))
        lane = lax.broadcasted_iota(jnp.int32, gates.shape, 1)
        share = jnp.where(lane >= n_real, MASK[m][:, :n_total] * gates, 0.0)
        ZS[m] = jnp.broadcast_to(jnp.sum(share, axis=-1, keepdims=True), (ROWS, LANES))

    def tokens(m, start, size):
        return G[m, :, :, :, :, pl.ds(start, size)].reshape(rows, size)

    def compute(m):
        hid = jnp.zeros((rows, 2 * LANES), F32)
        for p in range(3):
            hid += jnp.dot(tokens(m, offs[p], part), W1[pl.ds(offs[p], part)], preferred_element_type=F32)
        LH[:, 0:LANES] = (jax.nn.silu(hid[:, :LANES]) * hid[:, LANES:]).astype(BF16)
        codes = tokens(m, width, LANES)
        pick = (lax.broadcasted_iota(jnp.int32, (LANES, n_slots), 0) == group).astype(BF16)
        col = jnp.dot(codes, pick, preferred_element_type=F32)
        tok = lax.broadcasted_iota(jnp.int32, (rows, n_slots), 0)
        slot = lax.broadcasted_iota(jnp.int32, (rows, n_slots), 1)
        hit = (tok // ROWS == slot // slots) & (col == (slot % slots + 1).astype(F32))
        LH[:, LANES:] = jnp.where(hit, 1.0, 0.0).astype(BF16)
        pick_t = (lax.broadcasted_iota(jnp.int32, (ROWS, LANES), 1) == group).astype(BF16)
        row = lax.dot_general(pick_t, codes, (((1,), (1,)), ((), ())), preferred_element_type=F32)[0:1]
        slot = lax.broadcasted_iota(jnp.int32, (n_slots, rows), 0)
        tok = lax.broadcasted_iota(jnp.int32, (n_slots, rows), 1)
        hit = (tok // ROWS == slot // slots) & (row == (slot % slots + 1).astype(F32))
        chooser = jnp.where(hit, 1.0, 0.0).astype(BF16)
        for c in range(0, width, chunk):
            CH[:, pl.ds(c, chunk)] = jnp.dot(chooser, tokens(m, c, chunk), preferred_element_type=F32).astype(BF16)
        chosen = CH[...]
        logit = jnp.dot(chosen, RT[...], preferred_element_type=F32)
        lane = lax.broadcasted_iota(jnp.int32, logit.shape, 1)
        coef = jax.nn.sigmoid(jnp.sum(jnp.where(lane == group, logit, 0.0), axis=-1, keepdims=True))
        gate = jnp.dot(chosen, EG[...], preferred_element_type=F32)
        up = jnp.dot(chosen, EU[...], preferred_element_type=F32)
        inner = (jax.nn.silu(gate) * up).astype(BF16)
        for c in range(0, width, chunk):
            made = jnp.dot(inner, ED[:, pl.ds(c, chunk)], preferred_element_type=F32)
            DN[pl.ds(LANES, n_slots), pl.ds(c, chunk)] = (coef * made).astype(BF16)
        for p in range(3):
            for c in range(offs[p], offs[p] + part, chunk):
                both = jnp.dot(LH[...], DN[:, pl.ds(c, chunk)], preferred_element_type=F32).astype(BF16)
                PT[m, :, :, :, :, pl.ds(c, chunk)] = both.reshape(*sizes, ROWS, chunk)
            rs_start(m, p, 0)

    def rs_sum(m, p, s):
        axis = order[p][2 - s]
        n = sizes[axis]
        if s == 0:
            rest = [d for d in range(3) if d != axis]

            def add(i, carry):
                at = [slice(None)] * 3
                at[axis] = me[axis]
                at[rest[0]] = i
                total = PT[m, at[0], at[1], at[2], :, pl.ds(offs[p], part)].astype(F32)
                for o in range(n - 1):
                    total += R1[m, p, o, i].astype(F32)
                S1[m, p, i] = total.astype(BF16)
                return carry

            lax.fori_loop(0, sizes[rest[0]], add, 0)
        elif s == 1:
            rest = [d for d in range(3) if d != order[p][2]]
            at = [slice(None)] * 2
            at[rest.index(axis)] = me[axis]
            total = S1[m, p, at[0], at[1]].astype(F32)
            for o in range(n - 1):
                total += R2[m, p, o].astype(F32)
            S2[m, p] = total.astype(BF16)
        else:
            total = S2[m, p, me[axis]].astype(F32)
            for o in range(n - 1):
                total += R3[m, p, o].astype(F32)
            TS[m, :, pl.ds(offs[p], part)] = total.astype(BF16)

    def finish(m):
        tp_copy(m).wait_recv()
        normed = G[m, me[0], me[1], me[2], :, pl.ds(0, width)].astype(F32)
        summed = TS[m].astype(F32) + TR[m].astype(F32)
        done = (X[m].astype(F32) + summed + ZS[m][:, 0:1] * normed).astype(BF16)
        OB[m] = done
        out[0, m] = done[0:n_tok]

        @pl.when(sec == 0)
        def _():
            pp_copy(m).start()

    for m in range(n_micro):
        take_input(m)
        norm_and_send(m)
        if m == 0:
            for c in weight_copies():
                c.wait()
            W1[:, 0 : DG.shape[1]] = DG[...]
            W1[:, LANES : LANES + DU.shape[1]] = DU[...]
        zero_share(m)
        for s in range(3):
            for p in range(3):
                ag_wait(m, p, s)
                if s < 2:
                    ag_start(m, p, s + 1)
        compute(m)
        for s in range(3):
            for p in range(3):
                rs_wait(m, p, s)
                rs_sum(m, p, s)
                if s < 2:
                    rs_start(m, p, s + 1)
        tp_copy(m).start()
        finish(m)

    for m in range(n_micro):
        for p in range(3):
            for s in range(3):
                for o in range(1, sizes[order[p][s]]):
                    ag_copy(m, p, s, o).wait_send()
                for o in range(1, sizes[order[p][2 - s]]):
                    rs_copy(m, p, s, o).wait_send()
        tp_copy(m).wait_send()

        @pl.when(sec == 0)
        def _():
            pp_copy(m).wait_send()


def on_device(sizes, n_tp, acts, routes, gain, router, dg, du, dd, eg, eu, ed):
    n_micro, n_tok, width = acts.shape
    topk = routes.shape[-1]
    n_total = router.shape[-1]
    n_blocks = sizes[0] * sizes[1] * sizes[2]
    slots = max(2, (n_tok * topk + n_total - 1) // n_total)
    n_slots = n_blocks * slots
    part = width // 3
    chunk = min(512, part)
    n = sizes[0]
    inner = eg.shape[-1]
    cfg = (sizes, n_tp, width, n_micro, n_tok, topk, n_blocks, n_total, slots, chunk)
    vm = pltpu.VMEM
    scratch = [
        vm((n_micro, *sizes, ROWS, width + LANES), BF16),
        vm((n_micro, *sizes, ROWS, width), BF16),
        vm((n_micro, 3, n - 1, n, n, ROWS, part), BF16),
        vm((n_micro, 3, n, n, ROWS, part), BF16),
        vm((n_micro, 3, n - 1, n, ROWS, part), BF16),
        vm((n_micro, 3, n, ROWS, part), BF16),
        vm((n_micro, 3, n - 1, ROWS, part), BF16),
        vm((n_micro, ROWS, width), BF16),
        vm((n_micro, ROWS, width), BF16),
        vm((n_micro, ROWS, width), BF16),
        vm((n_micro, ROWS, width), BF16),
        vm((n_micro, ROWS, LANES), F32),
        vm((n_micro, ROWS, LANES), F32),
        vm((n_micro, ROWS, LANES), F32),
        vm((width, n_total), BF16),
        vm((width, dg.shape[-1]), BF16),
        vm((width, du.shape[-1]), BF16),
        vm((width, inner), BF16),
        vm((width, inner), BF16),
        vm((inner, width), BF16),
        vm((width, 2 * LANES), BF16),
        vm((n_blocks * ROWS, LANES + n_slots), BF16),
        vm((LANES + n_slots, width), BF16),
        vm((n_slots, width), BF16),
        pltpu.SemaphoreType.DMA((7,)),
        pltpu.SemaphoreType.DMA((n_micro, 3, 3, n - 1)),
        pltpu.SemaphoreType.DMA((n_micro, 3, 3, n - 1)),
        pltpu.SemaphoreType.DMA((n_micro, 3, 3, n - 1)),
        pltpu.SemaphoreType.DMA((n_micro, 3, 3, n - 1)),
        pltpu.SemaphoreType.DMA((n_micro,)),
        pltpu.SemaphoreType.DMA((n_micro,)),
        pltpu.SemaphoreType.DMA((n_micro,)),
        pltpu.SemaphoreType.DMA((n_micro,)),
    ]
    in_vmem = pl.BlockSpec(memory_space=pltpu.VMEM)
    left = pl.BlockSpec(memory_space=pl.ANY)
    return pl.pallas_call(
        functools.partial(kernel, cfg),
        out_shape=jax.ShapeDtypeStruct((1, n_micro, n_tok, width), BF16),
        in_specs=[in_vmem] * 3 + [left] * 7,
        out_specs=in_vmem,
        scratch_shapes=scratch,
        compiler_params=pltpu.CompilerParams(
            collective_id=0, has_side_effects=True, vmem_limit_bytes=60 * 1024 * 1024
        ),
        name="relay",
    )(acts, routes, gain, router, dg, du, dd, eg, eu, ed)


def solution(mesh):
    n_tp = mesh.shape["tp"]
    side = round(mesh.shape["ep"] ** (1 / 3))
    sizes = (side, side, side)
    finer = Mesh(
        mesh.devices.reshape(mesh.shape["pp"], *sizes, n_tp),
        ("pp", "ep_0", "ep_1", "ep_2", "tp"),
    )
    in_specs = (
        P(None, EP, None),
        P("pp", None, EP, None),
        P("pp", None),
        P("pp", None, None),
        P("pp", None, EP_TP),
        P("pp", None, EP_TP),
        P("pp", EP_TP, None),
        P("pp", EP, None, "tp"),
        P("pp", EP, None, "tp"),
        P("pp", EP, "tp", None),
    )
    return jax.shard_map(
        functools.partial(on_device, sizes, n_tp),
        mesh=finer,
        in_specs=in_specs,
        out_specs=P("pp", None, EP, None),
        check_vma=False,
    )
```

```python
import functools

import jax
import jax.numpy as jnp
from jax import lax
from jax.experimental import pallas as pl
from jax.experimental.pallas import tpu as pltpu
from jax.sharding import Mesh
from jax.sharding import PartitionSpec as P

MESH = pl.DeviceIdType.MESH
EP = ("ep_0", "ep_1", "ep_2")
EP_TP = ("ep_0", "ep_1", "ep_2", "tp")
F32 = jnp.float32
BF16 = jnp.bfloat16
ROWS = 8
LANES = 128


def dot_t(a, b):
    return lax.dot_general(a, b, (((1,), (1,)), ((), ())), preferred_element_type=F32)


def kernel(cfg, *refs):
    (acts, routes, gain, router_h, dg_h, du_h, dd_h, eg_h, eu_h, ed_h, out) = refs[:11]
    (G, PT, RA, RB, S1, R2, S2, R3, TS, TR, X, OB, CODE, MASK, ZS) = refs[11:26]
    (RT, EG, EU, ED, W1, LH, DN, CH) = refs[26:34]
    (w_sem, ag_s, ag_r, rs_s, rs_r, fa_s, fa_r, fr_s, fr_r, tp_s, tp_r, pp_s, pp_r) = refs[34:]
    sizes, n_tp, width, n_micro, n_tok, topk, n_real, n_total, slots, chunk = cfg
    n_blocks = sizes[0] * sizes[1] * sizes[2]
    rows = n_blocks * ROWS
    n_slots = n_blocks * slots
    part = width // 3
    offs = (0, part, 2 * part)
    gw = (part, part, part + LANES)
    order = ((0, 1, 2), (1, 2, 0), (2, 0, 1))

    sec = lax.axis_index("pp")
    me = tuple(lax.axis_index(a) for a in EP)
    tp = lax.axis_index("tp")
    group = (me[0] * sizes[1] + me[1]) * sizes[2] + me[2]

    def peer(axis, o):
        n = sizes[axis]
        if axis != 1:
            return {EP[axis]: lax.rem(me[axis] + o + n, n)}
        step = o if abs(o) <= n // 2 else o - n * (o // abs(o))
        z = lax.rem(tp * n + me[1] + step + n * n_tp, n * n_tp)
        return {"ep_1": lax.rem(z, n), "tp": z // n}

    far = {"tp": 1 - tp}
    above = {"pp": 1 - sec}

    def weight_copies():
        hidden = dg_h.shape[1]
        pairs = ((router_h.at[0], RT), (dg_h.at[0], W1.at[pl.ds(0, hidden)]), (du_h.at[0], W1.at[pl.ds(LANES, hidden)]),
                 (dd_h.at[0], DN.at[pl.ds(0, hidden)]),
                 (eg_h.at[0, 0], EG), (eu_h.at[0, 0], EU), (ed_h.at[0, 0], ED))
        return [pltpu.make_async_copy(s, d, w_sem.at[i]) for i, (s, d) in enumerate(pairs)]

    for c in weight_copies():
        c.start()

    X[...] = jnp.zeros_like(X)
    barrier = pltpu.get_barrier_semaphore()
    greeted = 0
    for axis in range(3):
        for o in range(1, sizes[axis]):
            pl.semaphore_signal(barrier, inc=1, device_id=peer(axis, -o), device_id_type=MESH)
            greeted += 1
    for who in (far, above):
        pl.semaphore_signal(barrier, inc=1, device_id=who, device_id_type=MESH)
        greeted += 1

    CODE[...] = jnp.zeros_like(CODE)
    MASK[...] = jnp.zeros_like(MASK)
    spare = LANES - dd_h.shape[1]
    for ref, start in ((W1, LANES - spare), (W1, 2 * LANES - spare), (DN, LANES - spare)):
        ref[pl.ds(start, spare)] = jnp.zeros((spare, width), BF16)
    for m in range(n_micro):
        ids = jnp.concatenate([routes[0, t, m : m + 1] for t in range(n_tok)], axis=0)
        lane = lax.broadcasted_iota(jnp.int32, (n_tok, LANES), 1)
        named = jnp.zeros((n_tok, LANES), F32)
        for k in range(topk):
            named += (ids[:, k : k + 1] == lane).astype(F32)
        MASK[m, 0:n_tok] = named
        before = jnp.zeros((1, LANES), F32)
        for t in range(n_tok):
            row = named[t : t + 1]
            CODE[m, t : t + 1] = row * (before + 1.0)
            before += row

    pl.semaphore_wait(barrier, greeted)

    def ag_copy(m, p, s, o):
        axes = order[p]
        at = [me[0], me[1], me[2]]
        for a in axes[:s]:
            at[a] = slice(None)
        ref = G.at[m, at[0], at[1], at[2], :, pl.ds(offs[p], gw[p])]
        return pltpu.make_async_remote_copy(
            src_ref=ref, dst_ref=ref, send_sem=ag_s.at[m, p, s, o - 1], recv_sem=ag_r.at[m, p, s, o - 1],
            device_id=peer(axes[s], o), device_id_type=MESH)

    def ag_start(m, p, s):
        for o in range(1, sizes[order[p][s]]):
            ag_copy(m, p, s, o).start()

    def ag_wait(m, p, s):
        for o in range(1, sizes[order[p][s]]):
            ag_copy(m, p, s, o).wait_recv()

    def rs_refs(m, p, s, o):
        axis = order[p][2 - s]
        there = lax.rem(me[axis] + o, sizes[axis])
        if s == 1:
            rest = [d for d in range(3) if d != order[p][2]]
            at = [slice(None)] * 2
            at[rest.index(axis)] = there
            return S1.at[m, p, at[0], at[1]], R2.at[m, p, o - 1]
        return S2.at[m, p, there], R3.at[m, p, o - 1]

    def rs_copy(m, p, s, o):
        src, dst = rs_refs(m, p, s, o)
        return pltpu.make_async_remote_copy(
            src_ref=src, dst_ref=dst, send_sem=rs_s.at[m, p, s - 1, o - 1], recv_sem=rs_r.at[m, p, s - 1, o - 1],
            device_id=peer(order[p][2 - s], o), device_id_type=MESH)

    def rs_start(m, p, s):
        for o in range(1, sizes[order[p][2 - s]]):
            rs_copy(m, p, s, o).start()

    def rs_wait(m, p, s):
        for o in range(1, sizes[order[p][2 - s]]):
            rs_copy(m, p, s, o).wait_recv()

    def plane(ref, m, axis, there, start, size):
        at = [slice(None)] * 3
        at[axis] = there
        return ref.at[m, at[0], at[1], at[2], :, pl.ds(start, size)]

    def far_gather(m, p, k):
        axis = order[p][2]
        right = k in (0, 2, 4)
        low = k in (0, 3, 4)
        owner = lax.rem(me[axis] + sizes[axis] + (-1 if k == 4 else 1 if k == 5 else 0), sizes[axis])
        half = part // 2
        ref = plane(G, m, axis, owner, offs[p] if low else offs[p] + half, half if low else gw[p] - half)
        return pltpu.make_async_remote_copy(
            src_ref=ref, dst_ref=ref, send_sem=fa_s.at[m, p, k], recv_sem=fa_r.at[m, p, k],
            device_id=peer(axis, 1 if right else -1), device_id_type=MESH)

    def far_reduce(m, p, k):
        axis = order[p][2]
        n = sizes[axis]
        right = k in (0, 2, 4)
        low = k in (0, 3, 4)
        half = part // 2
        there = lax.rem(me[axis] + (2 if k < 2 else 1 if right else n - 1), n)
        src = plane(PT, m, axis, there, offs[p] + (0 if low else half), half)
        side = 0 if right else 1
        dst = RA.at[m, p, side] if k < 2 else RB.at[m, p, side, :, :, :, pl.ds(0 if low else half, half)]
        return pltpu.make_async_remote_copy(
            src_ref=src, dst_ref=dst, send_sem=fr_s.at[m, p, k], recv_sem=fr_r.at[m, p, k],
            device_id=peer(axis, 1 if right else -1), device_id_type=MESH)

    def forward(m):
        for p in range(3):
            for k in (0, 1):
                far_gather(m, p, k).wait_recv()
                far_gather(m, p, k + 4).start()

    def merge(m):
        half = part // 2
        for p in range(3):
            axis = order[p][2]
            rest = [d for d in range(3) if d != axis]
            for k in (0, 1):
                far_reduce(m, p, k).wait_recv()
                there = lax.rem(me[axis] + (1 if k == 0 else sizes[axis] - 1), sizes[axis])

                def add(i, carry):
                    at = [slice(None)] * 3
                    at[axis] = there
                    at[rest[0]] = i
                    where = (m, at[0], at[1], at[2], slice(None), pl.ds(offs[p] + k * half, half))
                    PT[where] = (PT[where].astype(F32) + RA[m, p, k, i].astype(F32)).astype(BF16)
                    return carry

                lax.fori_loop(0, sizes[rest[0]], add, 0)
                far_reduce(m, p, k + 4).start()

    def tp_copy(m):
        return pltpu.make_async_remote_copy(
            src_ref=TS.at[m], dst_ref=TR.at[m], send_sem=tp_s.at[m], recv_sem=tp_r.at[m],
            device_id=far, device_id_type=MESH)

    def pp_copy(m):
        return pltpu.make_async_remote_copy(
            src_ref=OB.at[m], dst_ref=X.at[m], send_sem=pp_s.at[m], recv_sem=pp_r.at[m],
            device_id=above, device_id_type=MESH)

    def take_input(m):
        @pl.when(sec == 0)
        def _():
            for t in range(n_tok):
                X[m, t : t + 1] = acts[t, m : m + 1]

        @pl.when(sec == 1)
        def _():
            pp_copy(m).wait_recv()

    def norm_and_send(m):
        wide = X[m].astype(F32)
        spread = jnp.mean(wide * wide, axis=-1, keepdims=True)
        normed = (wide * lax.rsqrt(spread + 1e-06) * gain[...].astype(F32)).astype(BF16)
        G[m, me[0], me[1], me[2], :, pl.ds(0, width)] = normed
        G[m, me[0], me[1], me[2], :, pl.ds(width, LANES)] = CODE[m].astype(BF16)
        for p in range(3):
            ag_start(m, p, 0)

    def zero_share(m):
        normed = G[m, me[0], me[1], me[2], :, pl.ds(0, width)]
        gates = jax.nn.sigmoid(dot_t(normed, RT[...]))
        lane = lax.broadcasted_iota(jnp.int32, gates.shape, 1)
        share = jnp.where(lane >= n_real, MASK[m][:, :n_total] * gates, 0.0)
        ZS[m] = jnp.broadcast_to(jnp.sum(share, axis=-1, keepdims=True), (ROWS, LANES))

    def tokens(m, start, size):
        return G[m, :, :, :, :, pl.ds(start, size)].reshape(rows, size)

    def compute(m):
        hid = jnp.zeros((rows, 2 * LANES), F32)
        for p in range(3):
            hid += dot_t(tokens(m, offs[p], part), W1[:, pl.ds(offs[p], part)])
        LH[:, 0:LANES] = (jax.nn.silu(hid[:, :LANES]) * hid[:, LANES:]).astype(BF16)
        codes = tokens(m, width, LANES)
        pick = (lax.broadcasted_iota(jnp.int32, (LANES, n_slots), 0) == group).astype(BF16)
        col = jnp.dot(codes, pick, preferred_element_type=F32)
        tok = lax.broadcasted_iota(jnp.int32, (rows, n_slots), 0)
        slot = lax.broadcasted_iota(jnp.int32, (rows, n_slots), 1)
        hit = (tok // ROWS == slot // slots) & (col == (slot % slots + 1).astype(F32))
        LH[:, LANES:] = jnp.where(hit, 1.0, 0.0).astype(BF16)
        pick_t = (lax.broadcasted_iota(jnp.int32, (ROWS, LANES), 1) == group).astype(BF16)
        row = dot_t(pick_t, codes)[0:1]
        slot = lax.broadcasted_iota(jnp.int32, (n_slots, rows), 0)
        tok = lax.broadcasted_iota(jnp.int32, (n_slots, rows), 1)
        hit = (tok // ROWS == slot // slots) & (row == (slot % slots + 1).astype(F32))
        chooser = jnp.where(hit, 1.0, 0.0).astype(BF16)
        for c in range(0, width, chunk):
            CH[:, pl.ds(c, chunk)] = jnp.dot(chooser, tokens(m, c, chunk), preferred_element_type=F32).astype(BF16)
        chosen = CH[...]
        logit = dot_t(chosen, RT[...])
        lane = lax.broadcasted_iota(jnp.int32, logit.shape, 1)
        coef = jax.nn.sigmoid(jnp.sum(jnp.where(lane == group, logit, 0.0), axis=-1, keepdims=True))
        gate = jnp.dot(chosen, EG[...], preferred_element_type=F32)
        up = jnp.dot(chosen, EU[...], preferred_element_type=F32)
        inner = (jax.nn.silu(gate) * up).astype(BF16)
        for c in range(0, width, chunk):
            made = jnp.dot(inner, ED[:, pl.ds(c, chunk)], preferred_element_type=F32)
            DN[pl.ds(LANES, n_slots), pl.ds(c, chunk)] = (coef * made).astype(BF16)
        for p in range(3):
            for c in range(offs[p], offs[p] + part, chunk):
                both = jnp.dot(LH[...], DN[:, pl.ds(c, chunk)], preferred_element_type=F32).astype(BF16)
                PT[m, :, :, :, :, pl.ds(c, chunk)] = both.reshape(*sizes, ROWS, chunk)
            for k in range(4):
                far_reduce(m, p, k).start()

    def rs_sum(m, p, s):
        axis = order[p][2 - s]
        n = sizes[axis]
        if s == 0:
            rest = [d for d in range(3) if d != axis]

            def add(i, carry):
                at = [slice(None)] * 3
                at[axis] = me[axis]
                at[rest[0]] = i
                total = PT[m, at[0], at[1], at[2], :, pl.ds(offs[p], part)].astype(F32)
                for side in range(2):
                    total += RB[m, p, side, i].astype(F32)
                S1[m, p, i] = total.astype(BF16)
                return carry

            lax.fori_loop(0, sizes[rest[0]], add, 0)
        elif s == 1:
            rest = [d for d in range(3) if d != order[p][2]]
            at = [slice(None)] * 2
            at[rest.index(axis)] = me[axis]
            total = S1[m, p, at[0], at[1]].astype(F32)
            for o in range(n - 1):
                total += R2[m, p, o].astype(F32)
            S2[m, p] = total.astype(BF16)
        else:
            total = S2[m, p, me[axis]].astype(F32)
            for o in range(n - 1):
                total += R3[m, p, o].astype(F32)
            TS[m, :, pl.ds(offs[p], part)] = total.astype(BF16)

    def finish(m):
        tp_copy(m).wait_recv()
        normed = G[m, me[0], me[1], me[2], :, pl.ds(0, width)].astype(F32)
        summed = TS[m].astype(F32) + TR[m].astype(F32)
        done = (X[m].astype(F32) + summed + ZS[m][:, 0:1] * normed).astype(BF16)
        OB[m] = done
        for t in range(n_tok):
            out[0, t, m : m + 1] = done[t : t + 1]

        @pl.when(sec == 0)
        def _():
            pp_copy(m).start()

    def enter(m):
        take_input(m)
        norm_and_send(m)

    def gather(m, s):
        for p in range(3):
            if s < 2:
                ag_wait(m, p, s)
            else:
                for k in range(2, 6):
                    far_gather(m, p, k).wait_recv()
            if s == 0:
                ag_start(m, p, 1)
            elif s == 1:
                for k in range(4):
                    far_gather(m, p, k).start()

    def reduce(m, s):
        for p in range(3):
            if s == 0:
                for k in range(2, 6):
                    far_reduce(m, p, k).wait_recv()
            else:
                rs_wait(m, p, s)
            rs_sum(m, p, s)
            if s < 2:
                rs_start(m, p, s + 1)
        if s == 2:
            tp_copy(m).start()

    def only(section, *steps):
        @pl.when(sec == section)
        def _():
            for step in steps:
                step()

    enter(0)
    only(0, lambda: enter(1))
    gather(0, 0)
    gather(0, 1)
    only(0, lambda: gather(1, 0))
    forward(0)
    only(0, lambda: gather(1, 1))
    for c in weight_copies():
        c.wait()
    zero_share(0)
    gather(0, 2)
    compute(0)
    only(0, lambda: forward(1))
    merge(0)
    reduce(0, 0)
    only(1, lambda: enter(1))
    reduce(0, 1)
    only(1, lambda: gather(1, 0))
    reduce(0, 2)
    only(1, lambda: gather(1, 1))
    finish(0)
    only(1, lambda: forward(1))
    zero_share(1)
    gather(1, 2)
    compute(1)
    merge(1)
    for s in range(3):
        reduce(1, s)
    finish(1)

    for m in range(n_micro):
        for p in range(3):
            for s in range(2):
                for o in range(1, sizes[order[p][s]]):
                    ag_copy(m, p, s, o).wait_send()
                for o in range(1, sizes[order[p][1 - s]]):
                    rs_copy(m, p, s + 1, o).wait_send()
            for k in range(6):
                far_gather(m, p, k).wait_send()
                far_reduce(m, p, k).wait_send()
        tp_copy(m).wait_send()

        @pl.when(sec == 0)
        def _():
            pp_copy(m).wait_send()


def on_device(sizes, n_tp, acts, routes, gain, router, dg, du, dd, eg, eu, ed):
    swapped = (jnp.swapaxes(acts, 0, 1), jnp.swapaxes(routes, 1, 2), gain, *(jnp.swapaxes(w, 1, 2) for w in (router, dg, du)))
    return jnp.swapaxes(in_vmem(sizes, n_tp, *swapped, dd, eg, eu, ed), 1, 2)


def in_vmem(sizes, n_tp, acts, routes, gain, router, dg, du, dd, eg, eu, ed):
    n_tok, n_micro, width = acts.shape
    topk = routes.shape[-1]
    n_total = router.shape[1]
    n_blocks = sizes[0] * sizes[1] * sizes[2]
    slots = max(2, (n_tok * topk + n_total - 1) // n_total)
    n_slots = n_blocks * slots
    part = width // 3
    chunk = min(512, part)
    n = sizes[0]
    inner = eg.shape[-1]
    cfg = (sizes, n_tp, width, n_micro, n_tok, topk, n_blocks, n_total, slots, chunk)
    vm = pltpu.VMEM
    scratch = [
        vm((n_micro, *sizes, ROWS, width + LANES), BF16),
        vm((n_micro, *sizes, ROWS, width), BF16),
        vm((n_micro, 3, 2, n, n, ROWS, part // 2), BF16),
        vm((n_micro, 3, 2, n, n, ROWS, part), BF16),
        vm((n_micro, 3, n, n, ROWS, part), BF16),
        vm((n_micro, 3, n - 1, n, ROWS, part), BF16),
        vm((n_micro, 3, n, ROWS, part), BF16),
        vm((n_micro, 3, n - 1, ROWS, part), BF16),
        vm((n_micro, ROWS, width), BF16),
        vm((n_micro, ROWS, width), BF16),
        vm((n_micro, ROWS, width), BF16),
        vm((n_micro, ROWS, width), BF16),
        vm((n_micro, ROWS, LANES), F32),
        vm((n_micro, ROWS, LANES), F32),
        vm((n_micro, ROWS, LANES), F32),
        vm((n_total, width), BF16),
        vm((width, inner), BF16),
        vm((width, inner), BF16),
        vm((inner, width), BF16),
        vm((2 * LANES, width), BF16),
        vm((n_blocks * ROWS, LANES + n_slots), BF16),
        vm((LANES + n_slots, width), BF16),
        vm((n_slots, width), BF16),
        pltpu.SemaphoreType.DMA((7,)),
        pltpu.SemaphoreType.DMA((n_micro, 3, 2, n - 1)),
        pltpu.SemaphoreType.DMA((n_micro, 3, 2, n - 1)),
        pltpu.SemaphoreType.DMA((n_micro, 3, 2, n - 1)),
        pltpu.SemaphoreType.DMA((n_micro, 3, 2, n - 1)),
        pltpu.SemaphoreType.DMA((n_micro, 3, 6)),
        pltpu.SemaphoreType.DMA((n_micro, 3, 6)),
        pltpu.SemaphoreType.DMA((n_micro, 3, 6)),
        pltpu.SemaphoreType.DMA((n_micro, 3, 6)),
        pltpu.SemaphoreType.DMA((n_micro,)),
        pltpu.SemaphoreType.DMA((n_micro,)),
        pltpu.SemaphoreType.DMA((n_micro,)),
        pltpu.SemaphoreType.DMA((n_micro,)),
    ]
    held = pl.BlockSpec(memory_space=pltpu.VMEM)
    left = pl.BlockSpec(memory_space=pl.ANY)
    return pl.pallas_call(
        functools.partial(kernel, cfg),
        out_shape=jax.ShapeDtypeStruct((1, n_tok, n_micro, width), BF16),
        in_specs=[held] * 3 + [left] * 7,
        out_specs=held,
        scratch_shapes=scratch,
        compiler_params=pltpu.CompilerParams(
            collective_id=0, has_side_effects=True, vmem_limit_bytes=60 * 1024 * 1024
        ),
        name="relay",
    )(acts, routes, gain, router, dg, du, dd, eg, eu, ed)


def solution(mesh):
    n_tp = mesh.shape["tp"]
    side = round(mesh.shape["ep"] ** (1 / 3))
    sizes = (side, side, side)
    finer = Mesh(
        mesh.devices.reshape(mesh.shape["pp"], *sizes, n_tp),
        ("pp", "ep_0", "ep_1", "ep_2", "tp"),
    )
    in_specs = (
        P(None, EP, None),
        P("pp", None, EP, None),
        P("pp", None),
        P("pp", None, None),
        P("pp", None, EP_TP),
        P("pp", None, EP_TP),
        P("pp", EP_TP, None),
        P("pp", EP, None, "tp"),
        P("pp", EP, None, "tp"),
        P("pp", EP, "tp", None),
    )
    return jax.shard_map(
        functools.partial(on_device, sizes, n_tp),
        mesh=finer,
        in_specs=in_specs,
        out_specs=P("pp", None, EP, None),
        check_vma=False,
    )
```

```python
import functools

import jax
import jax.numpy as jnp
from jax import lax
from jax.experimental import pallas as pl
from jax.experimental.pallas import tpu as pltpu
from jax.sharding import Mesh
from jax.sharding import PartitionSpec as P

MESH = pl.DeviceIdType.MESH
EP = ("ep_0", "ep_1", "ep_2")
EP_TP = ("ep_0", "ep_1", "ep_2", "tp")
F32 = jnp.float32
BF16 = jnp.bfloat16
ROWS = 8
LANES = 128


def dot_t(a, b):
    return lax.dot_general(a, b, (((1,), (1,)), ((), ())), preferred_element_type=F32)


def kernel(cfg, *refs):
    (acts, routes, gain, router_h, dg_h, du_h, dd_h, eg_h, eu_h, ed_h, out) = refs[:11]
    (G, PT, RA, RB, S1, R2, S2, R3, TS, TR, X, OB, CODE, MASK, ZS) = refs[11:26]
    (RT, EG, EU, ED, W1, LH, DN, CH) = refs[26:34]
    (w_sem, ag_s, ag_r, rs_s, rs_r, fa_s, fa_r, fr_s, fr_r, tp_s, tp_r, pp_s, pp_r) = refs[34:]
    sizes, n_tp, width, n_micro, n_tok, topk, n_real, n_total, slots, chunk = cfg
    n_blocks = sizes[0] * sizes[1] * sizes[2]
    rows = n_blocks * ROWS
    n_slots = n_blocks * slots
    part = width // 3
    offs = (0, part, 2 * part)
    gw = (part, part, part + LANES)
    order = ((0, 1, 2), (1, 2, 0), (2, 0, 1))

    sec = lax.axis_index("pp")
    me = tuple(lax.axis_index(a) for a in EP)
    tp = lax.axis_index("tp")
    group = (me[0] * sizes[1] + me[1]) * sizes[2] + me[2]

    def peer(axis, o):
        n = sizes[axis]
        if axis != 1:
            return {EP[axis]: lax.rem(me[axis] + o + n, n)}
        step = o if abs(o) <= n // 2 else o - n * (o // abs(o))
        z = lax.rem(tp * n + me[1] + step + n * n_tp, n * n_tp)
        return {"ep_1": lax.rem(z, n), "tp": z // n}

    far = {"tp": 1 - tp}
    above = {"pp": 1 - sec}

    def weight_copies():
        hidden = dg_h.shape[1]
        pairs = ((router_h.at[0], RT), (dg_h.at[0], W1.at[pl.ds(0, hidden)]), (du_h.at[0], W1.at[pl.ds(LANES, hidden)]),
                 (dd_h.at[0], DN.at[pl.ds(0, hidden)]),
                 (eg_h.at[0, 0], EG), (eu_h.at[0, 0], EU), (ed_h.at[0, 0], ED))
        return [pltpu.make_async_copy(s, d, w_sem.at[i]) for i, (s, d) in enumerate(pairs)]

    for c in weight_copies():
        c.start()

    X[...] = jnp.zeros_like(X)
    barrier = pltpu.get_barrier_semaphore()
    greeted = 0
    for axis in range(3):
        for o in range(1, sizes[axis]):
            pl.semaphore_signal(barrier, inc=1, device_id=peer(axis, -o), device_id_type=MESH)
            greeted += 1
    pl.semaphore_signal(barrier, inc=1, device_id=above, device_id_type=MESH)
    greeted += 1

    CODE[...] = jnp.zeros_like(CODE)
    MASK[...] = jnp.zeros_like(MASK)
    spare = LANES - dd_h.shape[1]
    for ref, start in ((W1, LANES - spare), (W1, 2 * LANES - spare), (DN, LANES - spare)):
        ref[pl.ds(start, spare)] = jnp.zeros((spare, width), BF16)
    for m in range(n_micro):
        ids = jnp.concatenate([routes[0, t, m : m + 1] for t in range(n_tok)], axis=0)
        lane = lax.broadcasted_iota(jnp.int32, (n_tok, LANES), 1)
        named = jnp.zeros((n_tok, LANES), F32)
        for k in range(topk):
            named += (ids[:, k : k + 1] == lane).astype(F32)
        MASK[m, 0:n_tok] = named
        before = jnp.zeros((1, LANES), F32)
        for t in range(n_tok):
            row = named[t : t + 1]
            CODE[m, t : t + 1] = row * (before + 1.0)
            before += row

    pl.semaphore_wait(barrier, greeted)

    def ag_copy(m, p, s, o):
        axes = order[p]
        at = [me[0], me[1], me[2]]
        for a in axes[:s]:
            at[a] = slice(None)
        ref = G.at[m, at[0], at[1], at[2], :, pl.ds(offs[p], gw[p])]
        return pltpu.make_async_remote_copy(
            src_ref=ref, dst_ref=ref, send_sem=ag_s.at[m, p, s, o - 1], recv_sem=ag_r.at[m, p, s, o - 1],
            device_id=peer(axes[s], o), device_id_type=MESH)

    def ag_start(m, p, s):
        for o in range(1, sizes[order[p][s]]):
            ag_copy(m, p, s, o).start()

    def ag_wait(m, p, s):
        for o in range(1, sizes[order[p][s]]):
            ag_copy(m, p, s, o).wait_recv()

    def rs_refs(m, p, s, o):
        axis = order[p][2 - s]
        there = lax.rem(me[axis] + o, sizes[axis])
        if s == 1:
            rest = [d for d in range(3) if d != order[p][2]]
            at = [slice(None)] * 2
            at[rest.index(axis)] = there
            return S1.at[m, p, at[0], at[1]], R2.at[m, p, o - 1]
        return S2.at[m, p, there], R3.at[m, p, o - 1]

    def rs_copy(m, p, s, o):
        src, dst = rs_refs(m, p, s, o)
        return pltpu.make_async_remote_copy(
            src_ref=src, dst_ref=dst, send_sem=rs_s.at[m, p, s - 1, o - 1], recv_sem=rs_r.at[m, p, s - 1, o - 1],
            device_id=peer(order[p][2 - s], o), device_id_type=MESH)

    def rs_start(m, p, s):
        for o in range(1, sizes[order[p][2 - s]]):
            rs_copy(m, p, s, o).start()

    def rs_wait(m, p, s):
        for o in range(1, sizes[order[p][2 - s]]):
            rs_copy(m, p, s, o).wait_recv()

    def plane(ref, m, axis, there, start, size):
        at = [slice(None)] * 3
        at[axis] = there
        return ref.at[m, at[0], at[1], at[2], :, pl.ds(start, size)]

    half, quarter = part // 2, part // 4

    def lanes_of(p, way, k, width_p):
        if k == 2:
            return ((1 - way) * half, half if way == 1 else width_p - half)
        start = way * half + (k % 3) * quarter
        return (start, width_p - start if way == 1 and k % 3 == 1 else quarter)

    def far_gather(m, p, way, k):
        axis = order[p][2]
        shift = 0 if k < 3 else (-1, 1)[way]
        start, size = lanes_of(p, way, k, gw[p])
        ref = plane(G, m, axis, lax.rem(me[axis] + sizes[axis] + shift, sizes[axis]), offs[p] + start, size)
        return pltpu.make_async_remote_copy(
            src_ref=ref, dst_ref=ref, send_sem=fa_s.at[m, p, way, k], recv_sem=fa_r.at[m, p, way, k],
            device_id=peer(axis, (1, -1)[way]), device_id_type=MESH)

    def far_reduce(m, p, way, k):
        axis = order[p][2]
        n = sizes[axis]
        start, size = lanes_of(p, way, k, part)
        src = plane(PT, m, axis, lax.rem(me[axis] + (2 if k < 2 else (1, n - 1)[way]), n), offs[p] + start, size)
        if k < 2:
            dst = RA.at[m, p, way, :, :, :, pl.ds(k * quarter, quarter)]
        else:
            dst = RB.at[m, p, way, :, :, :, pl.ds(start, size)]
        return pltpu.make_async_remote_copy(
            src_ref=src, dst_ref=dst, send_sem=fr_s.at[m, p, way, k], recv_sem=fr_r.at[m, p, way, k],
            device_id=peer(axis, (1, -1)[way]), device_id_type=MESH)

    def far_start(copy, m, p):
        for k in range(3):
            for way in range(2):
                copy(m, p, way, k).start()

    def far_wait(copy, m, p):
        for k in range(2, 5):
            for way in range(2):
                copy(m, p, way, k).wait_recv()

    def forward(m):
        for k in range(2):
            for p in range(3):
                for way in range(2):
                    far_gather(m, p, way, k).wait_recv()
                    far_gather(m, p, way, k + 3).start()

    def merge(m):
        for k in range(2):
            for p in range(3):
                axis = order[p][2]
                rest = [d for d in range(3) if d != axis]
                for way in range(2):
                    far_reduce(m, p, way, k).wait_recv()
                    at = [slice(None)] * 3
                    at[axis] = lax.rem(me[axis] + (1, sizes[axis] - 1)[way], sizes[axis])
                    where = (m, *at, slice(None), pl.ds(offs[p] + way * half + k * quarter, quarter))
                    come = RA[m, p, way, :, :, :, pl.ds(k * quarter, quarter)].astype(F32)
                    PT[where] = (PT[where].astype(F32) + come).astype(BF16)
                    far_reduce(m, p, way, k + 3).start()

    def tp_copy(m, p):
        lanes = pl.ds(offs[p], part)
        return pltpu.make_async_remote_copy(
            src_ref=TS.at[m, :, lanes], dst_ref=TR.at[m, :, lanes], send_sem=tp_s.at[m, p], recv_sem=tp_r.at[m, p],
            device_id=far, device_id_type=MESH)

    def pp_copy(m):
        return pltpu.make_async_remote_copy(
            src_ref=OB.at[m], dst_ref=X.at[m], send_sem=pp_s.at[m], recv_sem=pp_r.at[m],
            device_id=above, device_id_type=MESH)

    def take_input(m):
        @pl.when(sec == 0)
        def _():
            for t in range(n_tok):
                X[m, t : t + 1] = acts[t, m : m + 1]

        @pl.when(sec == 1)
        def _():
            pp_copy(m).wait_recv()

    def norm_and_send(m):
        wide = X[m].astype(F32)
        spread = jnp.mean(wide * wide, axis=-1, keepdims=True)
        normed = (wide * lax.rsqrt(spread + 1e-06) * gain[...].astype(F32)).astype(BF16)
        G[m, me[0], me[1], me[2], :, pl.ds(0, width)] = normed
        G[m, me[0], me[1], me[2], :, pl.ds(width, LANES)] = CODE[m].astype(BF16)
        for p in range(3):
            ag_start(m, p, 0)

    def zero_share(m):
        normed = G[m, me[0], me[1], me[2], :, pl.ds(0, width)]
        gates = jax.nn.sigmoid(dot_t(normed, RT[...]))
        lane = lax.broadcasted_iota(jnp.int32, gates.shape, 1)
        share = jnp.where(lane >= n_real, MASK[m][:, :n_total] * gates, 0.0)
        ZS[m] = jnp.broadcast_to(jnp.sum(share, axis=-1, keepdims=True), (ROWS, LANES))

    def tokens(m, start, size):
        return G[m, :, :, :, :, pl.ds(start, size)].reshape(rows, size)

    def work(m):
        hid = jnp.zeros((rows, 2 * LANES), F32)
        for p in range(3):
            hid += dot_t(tokens(m, offs[p], part), W1[:, pl.ds(offs[p], part)])
        LH[:, 0:LANES] = (jax.nn.silu(hid[:, :LANES]) * hid[:, LANES:]).astype(BF16)
        codes = tokens(m, width, LANES)
        pick = (lax.broadcasted_iota(jnp.int32, (LANES, n_slots), 0) == group).astype(BF16)
        col = jnp.dot(codes, pick, preferred_element_type=F32)
        tok = lax.broadcasted_iota(jnp.int32, (rows, n_slots), 0)
        slot = lax.broadcasted_iota(jnp.int32, (rows, n_slots), 1)
        hit = (tok // ROWS == slot // slots) & (col == (slot % slots + 1).astype(F32))
        LH[:, LANES:] = jnp.where(hit, 1.0, 0.0).astype(BF16)
        pick_t = (lax.broadcasted_iota(jnp.int32, (ROWS, LANES), 1) == group).astype(BF16)
        row = dot_t(pick_t, codes)[0:1]
        slot = lax.broadcasted_iota(jnp.int32, (n_slots, rows), 0)
        tok = lax.broadcasted_iota(jnp.int32, (n_slots, rows), 1)
        hit = (tok // ROWS == slot // slots) & (row == (slot % slots + 1).astype(F32))
        chooser = jnp.where(hit, 1.0, 0.0).astype(BF16)
        for c in range(0, width, chunk):
            CH[:, pl.ds(c, chunk)] = jnp.dot(chooser, tokens(m, c, chunk), preferred_element_type=F32).astype(BF16)
        chosen = CH[...]
        logit = dot_t(chosen, RT[...])
        lane = lax.broadcasted_iota(jnp.int32, logit.shape, 1)
        coef = jax.nn.sigmoid(jnp.sum(jnp.where(lane == group, logit, 0.0), axis=-1, keepdims=True))
        gate = jnp.dot(chosen, EG[...], preferred_element_type=F32)
        up = jnp.dot(chosen, EU[...], preferred_element_type=F32)
        inner = (jax.nn.silu(gate) * up).astype(BF16)
        for c in range(0, width, chunk):
            made = jnp.dot(inner, ED[:, pl.ds(c, chunk)], preferred_element_type=F32)
            DN[pl.ds(LANES, n_slots), pl.ds(c, chunk)] = (coef * made).astype(BF16)

    def put_out(m):
        for p in range(3):
            for c in range(offs[p], offs[p] + part, chunk):
                both = jnp.dot(LH[...], DN[:, pl.ds(c, chunk)], preferred_element_type=F32).astype(BF16)
                PT[m, :, :, :, :, pl.ds(c, chunk)] = both.reshape(*sizes, ROWS, chunk)
            far_start(far_reduce, m, p)

    def rs_sum(m, p, s):
        axis = order[p][2 - s]
        n = sizes[axis]
        if s == 0:
            rest = [d for d in range(3) if d != axis]

            def add(i, carry):
                at = [slice(None)] * 3
                at[axis] = me[axis]
                at[rest[0]] = i
                total = PT[m, at[0], at[1], at[2], :, pl.ds(offs[p], part)].astype(F32)
                for side in range(2):
                    total += RB[m, p, side, i].astype(F32)
                S1[m, p, i] = total.astype(BF16)
                return carry

            lax.fori_loop(0, sizes[rest[0]], add, 0)
        elif s == 1:
            rest = [d for d in range(3) if d != order[p][2]]
            at = [slice(None)] * 2
            at[rest.index(axis)] = me[axis]
            total = S1[m, p, at[0], at[1]].astype(F32)
            for o in range(n - 1):
                total += R2[m, p, o].astype(F32)
            S2[m, p] = total.astype(BF16)
        else:
            total = S2[m, p, me[axis]].astype(F32)
            for o in range(n - 1):
                total += R3[m, p, o].astype(F32)
            TS[m, :, pl.ds(offs[p], part)] = total.astype(BF16)

    def finish(m):
        for p in range(3):
            tp_copy(m, p).wait_recv()
        normed = G[m, me[0], me[1], me[2], :, pl.ds(0, width)].astype(F32)
        summed = TS[m].astype(F32) + TR[m].astype(F32)
        done = (X[m].astype(F32) + summed + ZS[m][:, 0:1] * normed).astype(BF16)
        OB[m] = done
        for t in range(n_tok):
            out[0, t, m : m + 1] = done[t : t + 1]

        @pl.when(sec == 0)
        def _():
            pp_copy(m).start()

    def enter(m):
        take_input(m)
        norm_and_send(m)

    def gather(m, s):
        for p in range(3):
            if s < 2:
                ag_wait(m, p, s)
            else:
                far_wait(far_gather, m, p)
            if s == 0:
                ag_start(m, p, 1)
            elif s == 1:
                far_start(far_gather, m, p)

    def reduce(m, s):
        for p in range(3):
            if s == 0:
                far_wait(far_reduce, m, p)
            else:
                rs_wait(m, p, s)
            rs_sum(m, p, s)
            if s < 2:
                rs_start(m, p, s + 1)
            else:
                tp_copy(m, p).start()

    def only(section, *steps):
        @pl.when(sec == section)
        def _():
            for step in steps:
                step()

    enter(0)
    only(0, lambda: enter(1))
    gather(0, 0)
    only(1, lambda: enter(1))
    gather(1, 0)
    gather(0, 1)
    forward(0)
    gather(1, 1)
    for c in weight_copies():
        c.wait()
    zero_share(0)
    gather(0, 2)
    forward(1)
    work(0)
    put_out(0)
    zero_share(1)
    gather(1, 2)
    work(1)
    merge(0)
    put_out(1)
    merge(1)
    reduce(0, 0)
    reduce(1, 0)
    reduce(0, 1)
    reduce(1, 1)
    reduce(0, 2)
    reduce(1, 2)
    finish(0)
    finish(1)

    for m in range(n_micro):
        for p in range(3):
            for s in range(2):
                for o in range(1, sizes[order[p][s]]):
                    ag_copy(m, p, s, o).wait_send()
                for o in range(1, sizes[order[p][1 - s]]):
                    rs_copy(m, p, s + 1, o).wait_send()
            for k in range(5):
                for way in range(2):
                    far_gather(m, p, way, k).wait_send()
                    far_reduce(m, p, way, k).wait_send()
            tp_copy(m, p).wait_send()
        @pl.when(sec == 0)
        def _():
            pp_copy(m).wait_send()


def on_device(sizes, n_tp, acts, routes, gain, router, dg, du, dd, eg, eu, ed):
    swapped = (jnp.swapaxes(acts, 0, 1), jnp.swapaxes(routes, 1, 2), gain, *(jnp.swapaxes(w, 1, 2) for w in (router, dg, du)))
    return jnp.swapaxes(in_vmem(sizes, n_tp, *swapped, dd, eg, eu, ed), 1, 2)


def in_vmem(sizes, n_tp, acts, routes, gain, router, dg, du, dd, eg, eu, ed):
    n_tok, n_micro, width = acts.shape
    topk = routes.shape[-1]
    n_total = router.shape[1]
    n_blocks = sizes[0] * sizes[1] * sizes[2]
    slots = max(2, (n_tok * topk + n_total - 1) // n_total)
    n_slots = n_blocks * slots
    part = width // 3
    chunk = min(512, part)
    n = sizes[0]
    inner = eg.shape[-1]
    cfg = (sizes, n_tp, width, n_micro, n_tok, topk, n_blocks, n_total, slots, chunk)
    vm = pltpu.VMEM
    scratch = [
        vm((n_micro, *sizes, ROWS, width + LANES), BF16),
        vm((n_micro, *sizes, ROWS, width), BF16),
        vm((n_micro, 3, 2, n, n, ROWS, part // 2), BF16),
        vm((n_micro, 3, 2, n, n, ROWS, part), BF16),
        vm((n_micro, 3, n, n, ROWS, part), BF16),
        vm((n_micro, 3, n - 1, n, ROWS, part), BF16),
        vm((n_micro, 3, n, ROWS, part), BF16),
        vm((n_micro, 3, n - 1, ROWS, part), BF16),
        vm((n_micro, ROWS, width), BF16),
        vm((n_micro, ROWS, width), BF16),
        vm((n_micro, ROWS, width), BF16),
        vm((n_micro, ROWS, width), BF16),
        vm((n_micro, ROWS, LANES), F32),
        vm((n_micro, ROWS, LANES), F32),
        vm((n_micro, ROWS, LANES), F32),
        vm((n_total, width), BF16),
        vm((width, inner), BF16),
        vm((width, inner), BF16),
        vm((inner, width), BF16),
        vm((2 * LANES, width), BF16),
        vm((n_blocks * ROWS, LANES + n_slots), BF16),
        vm((LANES + n_slots, width), BF16),
        vm((n_slots, width), BF16),
        pltpu.SemaphoreType.DMA((7,)),
        pltpu.SemaphoreType.DMA((n_micro, 3, 2, n - 1)),
        pltpu.SemaphoreType.DMA((n_micro, 3, 2, n - 1)),
        pltpu.SemaphoreType.DMA((n_micro, 3, 2, n - 1)),
        pltpu.SemaphoreType.DMA((n_micro, 3, 2, n - 1)),
        pltpu.SemaphoreType.DMA((n_micro, 3, 2, 5)),
        pltpu.SemaphoreType.DMA((n_micro, 3, 2, 5)),
        pltpu.SemaphoreType.DMA((n_micro, 3, 2, 5)),
        pltpu.SemaphoreType.DMA((n_micro, 3, 2, 5)),
        pltpu.SemaphoreType.DMA((n_micro, 3)),
        pltpu.SemaphoreType.DMA((n_micro, 3)),
        pltpu.SemaphoreType.DMA((n_micro,)),
        pltpu.SemaphoreType.DMA((n_micro,)),
    ]
    held = pl.BlockSpec(memory_space=pltpu.VMEM)
    left = pl.BlockSpec(memory_space=pltpu.HBM)
    return pl.pallas_call(
        functools.partial(kernel, cfg),
        out_shape=jax.ShapeDtypeStruct((1, n_tok, n_micro, width), BF16),
        in_specs=[held] * 3 + [left] * 7,
        out_specs=held,
        scratch_shapes=scratch,
        compiler_params=pltpu.CompilerParams(
            collective_id=0, has_side_effects=True, vmem_limit_bytes=60 * 1024 * 1024
        ),
        name="relay",
    )(acts, routes, gain, router, dg, du, dd, eg, eu, ed)


def solution(mesh):
    n_tp = mesh.shape["tp"]
    side = round(mesh.shape["ep"] ** (1 / 3))
    sizes = (side, side, side)
    finer = Mesh(
        mesh.devices.reshape(mesh.shape["pp"], *sizes, n_tp),
        ("pp", "ep_0", "ep_1", "ep_2", "tp"),
    )
    in_specs = (
        P(None, EP, None),
        P("pp", None, EP, None),
        P("pp", None),
        P("pp", None, None),
        P("pp", None, EP_TP),
        P("pp", None, EP_TP),
        P("pp", EP_TP, None),
        P("pp", EP, None, "tp"),
        P("pp", EP, None, "tp"),
        P("pp", EP, "tp", None),
    )
    return jax.shard_map(
        functools.partial(on_device, sizes, n_tp),
        mesh=finer,
        in_specs=in_specs,
        out_specs=P("pp", None, EP, None),
        check_vma=False,
    )
```

```python
import functools

import jax
import jax.numpy as jnp
from jax import lax
from jax.experimental import pallas as pl
from jax.experimental.pallas import tpu as pltpu
from jax.sharding import Mesh
from jax.sharding import PartitionSpec as P

MESH = pl.DeviceIdType.MESH
EP = ("ep_0", "ep_1", "ep_2")
EP_TP = ("ep_0", "ep_1", "ep_2", "tp")
F32 = jnp.float32
BF16 = jnp.bfloat16
ROWS = 8
LANES = 128


def farthest_first(n):
    return sorted(range(1, n), key=lambda o: -min(o, n - o))


def dot_t(a, b):
    return lax.dot_general(a, b, (((1,), (1,)), ((), ())), preferred_element_type=F32)


def kernel(cfg, *refs):
    (acts, routes, gain, router_h, dg_h, du_h, dd_h, eg_h, eu_h, ed_h, out) = refs[:11]
    (G, PT, RA, RB, S1, R2, S2, R3, TS, TR, TL, BASE, BL, X, OB, CODE, MASK) = refs[11:28]
    (RT, EG, EU, ED, W1, LH, DN, CH) = refs[28:36]
    (w_sem, ag_s, ag_r, rs_s, rs_r, fa_s, fa_r, fr_s, fr_r, tp_s, tp_r, tl_s, tl_r, pp_s, pp_r) = refs[36:]
    sizes, n_tp, width, n_micro, n_tok, topk, n_real, n_total, slots, chunk = cfg
    n_blocks = sizes[0] * sizes[1] * sizes[2]
    rows = n_blocks * ROWS
    n_slots = n_blocks * slots
    part = width // 3
    offs = (0, part, 2 * part)
    gw = (part, part, part + LANES)
    order = ((0, 1, 2), (1, 2, 0), (2, 0, 1))

    sec = lax.axis_index("pp")
    me = tuple(lax.axis_index(a) for a in EP)
    tp = lax.axis_index("tp")
    group = (me[0] * sizes[1] + me[1]) * sizes[2] + me[2]

    def peer(axis, o):
        n = sizes[axis]
        if axis != 1:
            return {EP[axis]: lax.rem(me[axis] + o + n, n)}
        step = o if abs(o) <= n // 2 else o - n * (o // abs(o))
        z = lax.rem(tp * n + me[1] + step + n * n_tp, n * n_tp)
        return {"ep_1": lax.rem(z, n), "tp": z // n}

    far_last = {"tp": 1 - tp, "pp": 1}
    above = {"pp": 1 - sec}

    def weight_copies():
        hidden = dg_h.shape[1]
        pairs = ((router_h.at[0], RT), (dg_h.at[0], W1.at[pl.ds(0, hidden)]), (du_h.at[0], W1.at[pl.ds(LANES, hidden)]),
                 (dd_h.at[0], DN.at[pl.ds(0, hidden)]),
                 (eg_h.at[0, 0], EG), (eu_h.at[0, 0], EU), (ed_h.at[0, 0], ED))
        return [pltpu.make_async_copy(s, d, w_sem.at[i]) for i, (s, d) in enumerate(pairs)]

    for c in weight_copies():
        c.start()

    X[...] = jnp.zeros_like(X)
    barrier = pltpu.get_barrier_semaphore()
    greeted = 0
    for axis in range(3):
        for o in range(1, sizes[axis]):
            pl.semaphore_signal(barrier, inc=1, device_id=peer(axis, -o), device_id_type=MESH)
            greeted += 1
    pl.semaphore_signal(barrier, inc=1, device_id=above, device_id_type=MESH)
    greeted += 1

    CODE[...] = jnp.zeros_like(CODE)
    MASK[...] = jnp.zeros_like(MASK)
    spare = LANES - dd_h.shape[1]
    for ref, start in ((W1, LANES - spare), (W1, 2 * LANES - spare), (DN, LANES - spare)):
        ref[pl.ds(start, spare)] = jnp.zeros((spare, width), BF16)
    for m in range(n_micro):
        ids = jnp.concatenate([routes[0, t, m : m + 1] for t in range(n_tok)], axis=0)
        lane = lax.broadcasted_iota(jnp.int32, (n_tok, LANES), 1)
        named = jnp.zeros((n_tok, LANES), F32)
        for k in range(topk):
            named += (ids[:, k : k + 1] == lane).astype(F32)
        MASK[m, 0:n_tok] = named
        before = jnp.zeros((1, LANES), F32)
        for t in range(n_tok):
            row = named[t : t + 1]
            CODE[m, t : t + 1] = row * (before + 1.0)
            before += row

    pl.semaphore_wait(barrier, greeted)

    def ag_copy(m, p, s, o):
        axes = order[p]
        at = [me[0], me[1], me[2]]
        for a in axes[:s]:
            at[a] = slice(None)
        ref = G.at[m, at[0], at[1], at[2], :, pl.ds(offs[p], gw[p])]
        return pltpu.make_async_remote_copy(
            src_ref=ref, dst_ref=ref, send_sem=ag_s.at[m, p, s, o - 1], recv_sem=ag_r.at[m, p, s, o - 1],
            device_id=peer(axes[s], o), device_id_type=MESH)

    def ag_start(m, p, s):
        for o in farthest_first(sizes[order[p][s]]):
            ag_copy(m, p, s, o).start()

    def ag_wait(m, p, s):
        for o in range(1, sizes[order[p][s]]):
            ag_copy(m, p, s, o).wait_recv()

    def rs_refs(m, p, s, o):
        axis = order[p][2 - s]
        there = lax.rem(me[axis] + o, sizes[axis])
        if s == 1:
            rest = [d for d in range(3) if d != order[p][2]]
            at = [slice(None)] * 2
            at[rest.index(axis)] = there
            return S1.at[m, p, at[0], at[1]], R2.at[m, p, o - 1]
        return S2.at[m, p, there], R3.at[m, p, o - 1]

    def rs_copy(m, p, s, o):
        src, dst = rs_refs(m, p, s, o)
        return pltpu.make_async_remote_copy(
            src_ref=src, dst_ref=dst, send_sem=rs_s.at[m, p, s - 1, o - 1], recv_sem=rs_r.at[m, p, s - 1, o - 1],
            device_id=peer(order[p][2 - s], o), device_id_type=MESH)

    def rs_start(m, p, s):
        for o in farthest_first(sizes[order[p][2 - s]]):
            rs_copy(m, p, s, o).start()

    def rs_wait(m, p, s):
        for o in range(1, sizes[order[p][2 - s]]):
            rs_copy(m, p, s, o).wait_recv()

    def plane(ref, m, axis, there, start, size):
        at = [slice(None)] * 3
        at[axis] = there
        return ref.at[m, at[0], at[1], at[2], :, pl.ds(start, size)]

    half, quarter = part // 2, part // 4

    def lanes_of(p, way, k, width_p):
        if k == 2:
            return ((1 - way) * half, half if way == 1 else width_p - half)
        start = way * half + (k % 3) * quarter
        return (start, width_p - start if way == 1 and k % 3 == 1 else quarter)

    def far_gather(m, p, way, k):
        axis = order[p][2]
        shift = 0 if k < 3 else (-1, 1)[way]
        start, size = lanes_of(p, way, k, gw[p])
        ref = plane(G, m, axis, lax.rem(me[axis] + sizes[axis] + shift, sizes[axis]), offs[p] + start, size)
        return pltpu.make_async_remote_copy(
            src_ref=ref, dst_ref=ref, send_sem=fa_s.at[m, p, way, k], recv_sem=fa_r.at[m, p, way, k],
            device_id=peer(axis, (1, -1)[way]), device_id_type=MESH)

    def far_reduce(m, p, way, k):
        axis = order[p][2]
        n = sizes[axis]
        start, size = lanes_of(p, way, k, part)
        src = plane(PT, m, axis, lax.rem(me[axis] + (2 if k < 2 else (1, n - 1)[way]), n), offs[p] + start, size)
        if k < 2:
            dst = RA.at[m, p, way, :, :, :, pl.ds(k * quarter, quarter)]
        else:
            dst = RB.at[m, p, way, :, :, :, pl.ds(start, size)]
        return pltpu.make_async_remote_copy(
            src_ref=src, dst_ref=dst, send_sem=fr_s.at[m, p, way, k], recv_sem=fr_r.at[m, p, way, k],
            device_id=peer(axis, (1, -1)[way]), device_id_type=MESH)

    def far_start(copy, m, p):
        for k in range(3):
            for way in range(2):
                copy(m, p, way, k).start()

    def far_wait(copy, m, p):
        for k in range(2, 5):
            for way in range(2):
                copy(m, p, way, k).wait_recv()

    def forward(m):
        for k in range(2):
            for p in range(3):
                for way in range(2):
                    far_gather(m, p, way, k).wait_recv()
                    far_gather(m, p, way, k + 3).start()

    def merge(m):
        for k in range(2):
            for p in range(3):
                axis = order[p][2]
                rest = [d for d in range(3) if d != axis]
                for way in range(2):
                    far_reduce(m, p, way, k).wait_recv()
                    at = [slice(None)] * 3
                    at[axis] = lax.rem(me[axis] + (1, sizes[axis] - 1)[way], sizes[axis])
                    where = (m, *at, slice(None), pl.ds(offs[p] + way * half + k * quarter, quarter))
                    come = RA[m, p, way, :, :, :, pl.ds(k * quarter, quarter)].astype(F32)
                    PT[where] = (PT[where].astype(F32) + come).astype(BF16)
                    far_reduce(m, p, way, k + 3).start()

    def tp_copy(m, p, section):
        lanes = pl.ds(offs[p], part)
        return pltpu.make_async_remote_copy(
            src_ref=TS.at[m, :, lanes], dst_ref=TR.at[section, m, :, lanes], send_sem=tp_s.at[m, p],
            recv_sem=tp_r.at[section, m, p], device_id=far_last, device_id_type=MESH)

    def own_copy(m, p):
        lanes = pl.ds(offs[p], part)
        return pltpu.make_async_remote_copy(
            src_ref=TS.at[m, :, lanes], dst_ref=TL.at[m, :, lanes], send_sem=tl_s.at[m, p], recv_sem=tl_r.at[m, p],
            device_id=above, device_id_type=MESH)

    def base_copy(m):
        return pltpu.make_async_remote_copy(
            src_ref=BASE.at[m], dst_ref=BL.at[m], send_sem=pp_s.at[0, m], recv_sem=pp_r.at[0, m],
            device_id=above, device_id_type=MESH)

    def back_copy(m):
        return pltpu.make_async_remote_copy(
            src_ref=X.at[m], dst_ref=OB.at[m], send_sem=pp_s.at[1, m], recv_sem=pp_r.at[1, m],
            device_id=above, device_id_type=MESH)

    def take_input(m):
        @pl.when(sec == 0)
        def _():
            for t in range(n_tok):
                X[m, t : t + 1] = acts[t, m : m + 1]

        @pl.when(sec == 1)
        def _():
            base_copy(m).wait_recv()
            for p in range(3):
                own_copy(m, p).wait_recv()
                tp_copy(m, p, 0).wait_recv()
            X[m] = (BL[m] + (TL[m].astype(F32) + TR[0, m].astype(F32))).astype(BF16)
            back_copy(m).start()

    def norm_and_send(m):
        wide = X[m].astype(F32)
        spread = jnp.mean(wide * wide, axis=-1, keepdims=True)
        normed = (wide * lax.rsqrt(spread + 1e-06) * gain[...].astype(F32)).astype(BF16)
        G[m, me[0], me[1], me[2], :, pl.ds(0, width)] = normed
        G[m, me[0], me[1], me[2], :, pl.ds(width, LANES)] = CODE[m].astype(BF16)
        for p in range(3):
            ag_start(m, p, 0)

    def zero_share(m):
        normed = G[m, me[0], me[1], me[2], :, pl.ds(0, width)]
        gates = jax.nn.sigmoid(dot_t(normed, RT[...]))
        lane = lax.broadcasted_iota(jnp.int32, gates.shape, 1)
        share = jnp.where(lane >= n_real, MASK[m][:, :n_total] * gates, 0.0)
        share = jnp.sum(share, axis=-1, keepdims=True)
        BASE[m] = X[m].astype(F32) + share * normed.astype(F32)

        @pl.when(sec == 0)
        def _():
            base_copy(m).start()

    def tokens(m, start, size):
        return G[m, :, :, :, :, pl.ds(start, size)].reshape(rows, size)

    def work(m):
        mid = rows // 2
        for h in range(2):
            some = G[m, h * (sizes[0] // 2) : (h + 1) * (sizes[0] // 2), :, :, :, pl.ds(0, width)].reshape(mid, width)
            hid = dot_t(some, W1[...])
            LH[h * mid : (h + 1) * mid, 0:LANES] = (jax.nn.silu(hid[:, :LANES]) * hid[:, LANES:]).astype(BF16)
        codes = tokens(m, width, LANES)
        pick = (lax.broadcasted_iota(jnp.int32, (LANES, n_slots), 0) == group).astype(BF16)
        col = jnp.dot(codes, pick, preferred_element_type=F32)
        tok = lax.broadcasted_iota(jnp.int32, (rows, n_slots), 0)
        slot = lax.broadcasted_iota(jnp.int32, (rows, n_slots), 1)
        hit = (tok // ROWS == slot // slots) & (col == (slot % slots + 1).astype(F32))
        LH[:, LANES:] = jnp.where(hit, 1.0, 0.0).astype(BF16)
        pick_t = (lax.broadcasted_iota(jnp.int32, (ROWS, LANES), 1) == group).astype(BF16)
        row = dot_t(pick_t, codes)[0:1]
        slot = lax.broadcasted_iota(jnp.int32, (n_slots, rows), 0)
        tok = lax.broadcasted_iota(jnp.int32, (n_slots, rows), 1)
        hit = (tok // ROWS == slot // slots) & (row == (slot % slots + 1).astype(F32))
        chooser = jnp.where(hit, 1.0, 0.0).astype(BF16)
        if m == 0:
            forward(1)
        for c in range(0, width, chunk):
            CH[:, pl.ds(c, chunk)] = jnp.dot(chooser, tokens(m, c, chunk), preferred_element_type=F32).astype(BF16)
        chosen = CH[...]
        logit = dot_t(chosen, RT[...])
        lane = lax.broadcasted_iota(jnp.int32, logit.shape, 1)
        coef = jax.nn.sigmoid(jnp.sum(jnp.where(lane == group, logit, 0.0), axis=-1, keepdims=True))
        gate = jnp.dot(chosen, EG[...], preferred_element_type=F32)
        up = jnp.dot(chosen, EU[...], preferred_element_type=F32)
        inner = (jax.nn.silu(gate) * up).astype(BF16)
        for c in range(0, width, chunk):
            made = jnp.dot(inner, ED[:, pl.ds(c, chunk)], preferred_element_type=F32)
            DN[pl.ds(LANES, n_slots), pl.ds(c, chunk)] = (coef * made).astype(BF16)

    def put_out(m):
        for p in range(3):
            for c in range(offs[p], offs[p] + part, chunk):
                both = jnp.dot(LH[...], DN[:, pl.ds(c, chunk)], preferred_element_type=F32).astype(BF16)
                PT[m, :, :, :, :, pl.ds(c, chunk)] = both.reshape(*sizes, ROWS, chunk)
            far_start(far_reduce, m, p)

    def rs_sum(m, p, s):
        axis = order[p][2 - s]
        n = sizes[axis]
        if s == 0:
            rest = [d for d in range(3) if d != axis]

            def add(i, carry):
                at = [slice(None)] * 3
                at[axis] = me[axis]
                at[rest[0]] = i
                total = PT[m, at[0], at[1], at[2], :, pl.ds(offs[p], part)].astype(F32)
                for side in range(2):
                    total += RB[m, p, side, i].astype(F32)
                S1[m, p, i] = total.astype(BF16)
                return carry

            lax.fori_loop(0, sizes[rest[0]], add, 0)
        elif s == 1:
            rest = [d for d in range(3) if d != order[p][2]]
            at = [slice(None)] * 2
            at[rest.index(axis)] = me[axis]
            total = S1[m, p, at[0], at[1]].astype(F32)
            for o in range(n - 1):
                total += R2[m, p, o].astype(F32)
            S2[m, p] = total.astype(BF16)
        else:
            total = S2[m, p, me[axis]].astype(F32)
            for o in range(n - 1):
                total += R3[m, p, o].astype(F32)
            TS[m, :, pl.ds(offs[p], part)] = total.astype(BF16)

    def finish(m):
        @pl.when(sec == 0)
        def _():
            back_copy(m).wait_recv()
            for t in range(n_tok):
                out[0, t, m : m + 1] = OB[m, t : t + 1]

        @pl.when(sec == 1)
        def _():
            for p in range(3):
                tp_copy(m, p, 1).wait_recv()
            done = (BASE[m] + (TS[m].astype(F32) + TR[1, m].astype(F32))).astype(BF16)
            for t in range(n_tok):
                out[0, t, m : m + 1] = done[t : t + 1]

    def enter(m):
        take_input(m)
        norm_and_send(m)

    def gather(m, s):
        for p in range(3):
            if s < 2:
                ag_wait(m, p, s)
            else:
                far_wait(far_gather, m, p)
            if s == 0:
                ag_start(m, p, 1)
            elif s == 1:
                far_start(far_gather, m, p)

    def reduce(m, s):
        for p in range(3):
            if s == 0:
                far_wait(far_reduce, m, p)
            else:
                rs_wait(m, p, s)
            rs_sum(m, p, s)
            if s < 2:
                rs_start(m, p, s + 1)
            else:
                tp_copy(m, p, sec).start()

                @pl.when(sec == 0)
                def _():
                    own_copy(m, p).start()

    def only(section, *steps):
        @pl.when(sec == section)
        def _():
            for step in steps:
                step()

    enter(0)
    only(0, lambda: enter(1))
    gather(0, 0)
    only(1, lambda: enter(1))
    gather(1, 0)
    gather(0, 1)
    forward(0)
    gather(1, 1)
    for c in weight_copies():
        c.wait()
    zero_share(0)
    zero_share(1)
    gather(0, 2)
    work(0)
    put_out(0)
    gather(1, 2)
    work(1)
    merge(0)
    put_out(1)
    merge(1)
    reduce(0, 0)
    reduce(1, 0)
    reduce(0, 1)
    reduce(1, 1)
    reduce(0, 2)
    reduce(1, 2)
    finish(0)
    finish(1)

    for m in range(n_micro):
        for p in range(3):
            for s in range(2):
                for o in range(1, sizes[order[p][s]]):
                    ag_copy(m, p, s, o).wait_send()
                for o in range(1, sizes[order[p][1 - s]]):
                    rs_copy(m, p, s + 1, o).wait_send()
            for k in range(5):
                for way in range(2):
                    far_gather(m, p, way, k).wait_send()
                    far_reduce(m, p, way, k).wait_send()
            tp_copy(m, p, sec).wait_send()

        @pl.when(sec == 0)
        def _():
            for p in range(3):
                own_copy(m, p).wait_send()
            base_copy(m).wait_send()

        @pl.when(sec == 1)
        def _():
            back_copy(m).wait_send()


def on_device(sizes, n_tp, acts, routes, gain, router, dg, du, dd, eg, eu, ed):
    swapped = (jnp.swapaxes(acts, 0, 1), jnp.swapaxes(routes, 1, 2), gain, *(jnp.swapaxes(w, 1, 2) for w in (router, dg, du)))
    return jnp.swapaxes(in_vmem(sizes, n_tp, *swapped, dd, eg, eu, ed), 1, 2)


def in_vmem(sizes, n_tp, acts, routes, gain, router, dg, du, dd, eg, eu, ed):
    n_tok, n_micro, width = acts.shape
    topk = routes.shape[-1]
    n_total = router.shape[1]
    n_blocks = sizes[0] * sizes[1] * sizes[2]
    slots = max(2, (n_tok * topk + n_total - 1) // n_total)
    n_slots = n_blocks * slots
    part = width // 3
    chunk = min(512, part)
    n = sizes[0]
    inner = eg.shape[-1]
    cfg = (sizes, n_tp, width, n_micro, n_tok, topk, n_blocks, n_total, slots, chunk)
    vm = pltpu.VMEM
    scratch = [
        vm((n_micro, *sizes, ROWS, width + LANES), BF16),
        vm((n_micro, *sizes, ROWS, width), BF16),
        vm((n_micro, 3, 2, n, n, ROWS, part // 2), BF16),
        vm((n_micro, 3, 2, n, n, ROWS, part), BF16),
        vm((n_micro, 3, n, n, ROWS, part), BF16),
        vm((n_micro, 3, n - 1, n, ROWS, part), BF16),
        vm((n_micro, 3, n, ROWS, part), BF16),
        vm((n_micro, 3, n - 1, ROWS, part), BF16),
        vm((n_micro, ROWS, width), BF16),
        vm((2, n_micro, ROWS, width), BF16),
        vm((n_micro, ROWS, width), BF16),
        vm((n_micro, ROWS, width), F32),
        vm((n_micro, ROWS, width), F32),
        vm((n_micro, ROWS, width), BF16),
        vm((n_micro, ROWS, width), BF16),
        vm((n_micro, ROWS, LANES), F32),
        vm((n_micro, ROWS, LANES), F32),
        vm((n_total, width), BF16),
        vm((width, inner), BF16),
        vm((width, inner), BF16),
        vm((inner, width), BF16),
        vm((2 * LANES, width), BF16),
        vm((n_blocks * ROWS, LANES + n_slots), BF16),
        vm((LANES + n_slots, width), BF16),
        vm((n_slots, width), BF16),
        pltpu.SemaphoreType.DMA((7,)),
        pltpu.SemaphoreType.DMA((n_micro, 3, 2, n - 1)),
        pltpu.SemaphoreType.DMA((n_micro, 3, 2, n - 1)),
        pltpu.SemaphoreType.DMA((n_micro, 3, 2, n - 1)),
        pltpu.SemaphoreType.DMA((n_micro, 3, 2, n - 1)),
        pltpu.SemaphoreType.DMA((n_micro, 3, 2, 5)),
        pltpu.SemaphoreType.DMA((n_micro, 3, 2, 5)),
        pltpu.SemaphoreType.DMA((n_micro, 3, 2, 5)),
        pltpu.SemaphoreType.DMA((n_micro, 3, 2, 5)),
        pltpu.SemaphoreType.DMA((n_micro, 3)),
        pltpu.SemaphoreType.DMA((2, n_micro, 3)),
        pltpu.SemaphoreType.DMA((n_micro, 3)),
        pltpu.SemaphoreType.DMA((n_micro, 3)),
        pltpu.SemaphoreType.DMA((2, n_micro)),
        pltpu.SemaphoreType.DMA((2, n_micro)),
    ]
    held = pl.BlockSpec(memory_space=pltpu.VMEM)
    left = pl.BlockSpec(memory_space=pltpu.HBM)
    return pl.pallas_call(
        functools.partial(kernel, cfg),
        out_shape=jax.ShapeDtypeStruct((1, n_tok, n_micro, width), BF16),
        in_specs=[held] * 3 + [left] * 7,
        out_specs=held,
        scratch_shapes=scratch,
        compiler_params=pltpu.CompilerParams(
            collective_id=0, has_side_effects=True, vmem_limit_bytes=60 * 1024 * 1024
        ),
        name="relay",
    )(acts, routes, gain, router, dg, du, dd, eg, eu, ed)


def solution(mesh):
    n_tp = mesh.shape["tp"]
    side = round(mesh.shape["ep"] ** (1 / 3))
    sizes = (side, side, side)
    finer = Mesh(
        mesh.devices.reshape(mesh.shape["pp"], *sizes, n_tp),
        ("pp", "ep_0", "ep_1", "ep_2", "tp"),
    )
    in_specs = (
        P(None, EP, None),
        P("pp", None, EP, None),
        P("pp", None),
        P("pp", None, None),
        P("pp", None, EP_TP),
        P("pp", None, EP_TP),
        P("pp", EP_TP, None),
        P("pp", EP, None, "tp"),
        P("pp", EP, None, "tp"),
        P("pp", EP, "tp", None),
    )
    return jax.shard_map(
        functools.partial(on_device, sizes, n_tp),
        mesh=finer,
        in_specs=in_specs,
        out_specs=P("pp", None, EP, None),
        check_vma=False,
    )
```

```python
import functools

import jax
import jax.numpy as jnp
from jax import lax
from jax.experimental import pallas as pl
from jax.experimental.pallas import tpu as pltpu
from jax.sharding import Mesh
from jax.sharding import PartitionSpec as P

MESH = pl.DeviceIdType.MESH
EP = ("ep_0", "ep_1", "ep_2")
EP_TP = ("ep_0", "ep_1", "ep_2", "tp")
F32 = jnp.float32
BF16 = jnp.bfloat16
ROWS = 8
LANES = 128


def farthest_first(n):
    return sorted(range(1, n), key=lambda o: -min(o, n - o))


def dot_t(a, b):
    return lax.dot_general(a, b, (((1,), (1,)), ((), ())), preferred_element_type=F32)


def kernel(cfg, *refs):
    (acts, routes, gain, router_h, dg_h, du_h, dd_h, eg_h, eu_h, ed_h, out) = refs[:11]
    (G, PT, RA, RB, S1, R2, S2, R3, TS, TR, TL, BASE, BL, X, OB, CODE, MASK) = refs[11:28]
    (RT, EG, EU, ED, W1, LH, DN, CH) = refs[28:36]
    (w_sem, ag_s, ag_r, rs_s, rs_r, fa_s, fa_r, fr_s, fr_r, tp_s, tp_r, tl_s, tl_r, pp_s, pp_r) = refs[36:]
    sizes, n_tp, width, n_micro, n_tok, topk, n_real, n_total, slots, chunk = cfg
    n_blocks = sizes[0] * sizes[1] * sizes[2]
    rows = n_blocks * ROWS
    n_slots = n_blocks * slots
    part = width // 3
    offs = (0, part, 2 * part)
    gw = (part, part, part + LANES)
    order = ((0, 1, 2), (1, 2, 0), (2, 0, 1))

    sec = lax.axis_index("pp")
    me = tuple(lax.axis_index(a) for a in EP)
    tp = lax.axis_index("tp")
    group = (me[0] * sizes[1] + me[1]) * sizes[2] + me[2]

    def peer(axis, o):
        n = sizes[axis]
        if axis != 1:
            return {EP[axis]: lax.rem(me[axis] + o + n, n)}
        step = o if abs(o) <= n // 2 else o - n * (o // abs(o))
        z = lax.rem(tp * n + me[1] + step + n * n_tp, n * n_tp)
        return {"ep_1": lax.rem(z, n), "tp": z // n}

    far_last = {"tp": 1 - tp, "pp": 1}
    above = {"pp": 1 - sec}

    def weight_copies():
        hidden = dg_h.shape[1]
        pairs = ((router_h.at[0], RT), (dg_h.at[0], W1.at[pl.ds(0, hidden)]), (du_h.at[0], W1.at[pl.ds(LANES, hidden)]),
                 (dd_h.at[0], DN.at[pl.ds(0, hidden)]),
                 (eg_h.at[0, 0], EG), (eu_h.at[0, 0], EU), (ed_h.at[0, 0], ED))
        return [pltpu.make_async_copy(s, d, w_sem.at[i]) for i, (s, d) in enumerate(pairs)]

    for c in weight_copies():
        c.start()

    X[...] = jnp.zeros_like(X)
    barrier = pltpu.get_barrier_semaphore()
    greeted = 0
    for axis in range(3):
        for o in range(1, sizes[axis]):
            pl.semaphore_signal(barrier, inc=1, device_id=peer(axis, -o), device_id_type=MESH)
            greeted += 1
    pl.semaphore_signal(barrier, inc=1, device_id=above, device_id_type=MESH)
    greeted += 1

    CODE[...] = jnp.zeros_like(CODE)
    MASK[...] = jnp.zeros_like(MASK)
    spare = LANES - dd_h.shape[1]
    for ref, start in ((W1, LANES - spare), (W1, 2 * LANES - spare), (DN, LANES - spare)):
        ref[pl.ds(start, spare)] = jnp.zeros((spare, width), BF16)
    for m in range(n_micro):
        ids = jnp.concatenate([routes[0, t, m : m + 1] for t in range(n_tok)], axis=0)
        lane = lax.broadcasted_iota(jnp.int32, (n_tok, LANES), 1)
        named = jnp.zeros((n_tok, LANES), F32)
        for k in range(topk):
            named += (ids[:, k : k + 1] == lane).astype(F32)
        MASK[m, 0:n_tok] = named
        before = jnp.zeros((1, LANES), F32)
        for t in range(n_tok):
            row = named[t : t + 1]
            CODE[m, t : t + 1] = row * (before + 1.0)
            before += row

    def ag_copy(m, p, s, o):
        axes = order[p]
        at = [me[0], me[1], me[2]]
        for a in axes[:s]:
            at[a] = slice(None)
        ref = G.at[m, at[0], at[1], at[2], :, pl.ds(offs[p], gw[p])]
        return pltpu.make_async_remote_copy(
            src_ref=ref, dst_ref=ref, send_sem=ag_s.at[m, p, s, o - 1], recv_sem=ag_r.at[m, p, s, o - 1],
            device_id=peer(axes[s], o), device_id_type=MESH)

    def ag_start(m, p, s):
        for o in farthest_first(sizes[order[p][s]]):
            ag_copy(m, p, s, o).start()

    def ag_wait(m, p, s):
        for o in range(1, sizes[order[p][s]]):
            ag_copy(m, p, s, o).wait_recv()

    def rs_refs(m, p, s, o):
        axis = order[p][2 - s]
        there = lax.rem(me[axis] + o, sizes[axis])
        if s == 1:
            rest = [d for d in range(3) if d != order[p][2]]
            at = [slice(None)] * 2
            at[rest.index(axis)] = there
            return S1.at[m, p, at[0], at[1]], R2.at[m, p, o - 1]
        return S2.at[m, p, there], R3.at[m, p, o - 1]

    def rs_copy(m, p, s, o):
        src, dst = rs_refs(m, p, s, o)
        return pltpu.make_async_remote_copy(
            src_ref=src, dst_ref=dst, send_sem=rs_s.at[m, p, s - 1, o - 1], recv_sem=rs_r.at[m, p, s - 1, o - 1],
            device_id=peer(order[p][2 - s], o), device_id_type=MESH)

    def rs_start(m, p, s):
        for o in farthest_first(sizes[order[p][2 - s]]):
            rs_copy(m, p, s, o).start()

    def rs_wait(m, p, s):
        for o in range(1, sizes[order[p][2 - s]]):
            rs_copy(m, p, s, o).wait_recv()

    def plane(ref, m, axis, there, start, size):
        at = [slice(None)] * 3
        at[axis] = there
        return ref.at[m, at[0], at[1], at[2], :, pl.ds(start, size)]

    half, quarter = part // 2, part // 4

    def lanes_of(p, way, k, width_p):
        if k == 2:
            return ((1 - way) * half, half if way == 1 else width_p - half)
        start = way * half + (k % 3) * quarter
        return (start, width_p - start if way == 1 and k % 3 == 1 else quarter)

    def far_gather(m, p, way, k):
        axis = order[p][2]
        shift = 0 if k < 3 else (-1, 1)[way]
        start, size = lanes_of(p, way, k, gw[p])
        ref = plane(G, m, axis, lax.rem(me[axis] + sizes[axis] + shift, sizes[axis]), offs[p] + start, size)
        return pltpu.make_async_remote_copy(
            src_ref=ref, dst_ref=ref, send_sem=fa_s.at[m, p, way, k], recv_sem=fa_r.at[m, p, way, k],
            device_id=peer(axis, (1, -1)[way]), device_id_type=MESH)

    def far_reduce(m, p, way, k):
        axis = order[p][2]
        n = sizes[axis]
        start, size = lanes_of(p, way, k, part)
        src = plane(PT, m, axis, lax.rem(me[axis] + (2 if k < 2 else (1, n - 1)[way]), n), offs[p] + start, size)
        if k < 2:
            dst = RA.at[m, p, way, :, :, :, pl.ds(k * quarter, quarter)]
        else:
            dst = RB.at[m, p, way, :, :, :, pl.ds(start, size)]
        return pltpu.make_async_remote_copy(
            src_ref=src, dst_ref=dst, send_sem=fr_s.at[m, p, way, k], recv_sem=fr_r.at[m, p, way, k],
            device_id=peer(axis, (1, -1)[way]), device_id_type=MESH)

    def far_start(copy, m, p):
        for k in range(3):
            for way in range(2):
                copy(m, p, way, k).start()

    def far_wait(copy, m, p):
        for k in range(2, 5):
            for way in range(2):
                copy(m, p, way, k).wait_recv()

    def forward(m):
        for k in range(2):
            for p in range(3):
                for way in range(2):
                    far_gather(m, p, way, k).wait_recv()
                    far_gather(m, p, way, k + 3).start()

    def merge(m):
        for k in range(2):
            for p in range(3):
                axis = order[p][2]
                rest = [d for d in range(3) if d != axis]
                for way in range(2):
                    far_reduce(m, p, way, k).wait_recv()
                    at = [slice(None)] * 3
                    at[axis] = lax.rem(me[axis] + (1, sizes[axis] - 1)[way], sizes[axis])
                    where = (m, *at, slice(None), pl.ds(offs[p] + way * half + k * quarter, quarter))
                    come = RA[m, p, way, :, :, :, pl.ds(k * quarter, quarter)].astype(F32)
                    PT[where] = (PT[where].astype(F32) + come).astype(BF16)
                    far_reduce(m, p, way, k + 3).start()

    def tp_copy(m, p, section):
        lanes = pl.ds(offs[p], part)
        return pltpu.make_async_remote_copy(
            src_ref=TS.at[m, :, lanes], dst_ref=TR.at[section, m, :, lanes], send_sem=tp_s.at[m, p],
            recv_sem=tp_r.at[section, m, p], device_id=far_last, device_id_type=MESH)

    def own_copy(m, p):
        lanes = pl.ds(offs[p], part)
        return pltpu.make_async_remote_copy(
            src_ref=TS.at[m, :, lanes], dst_ref=TL.at[m, :, lanes], send_sem=tl_s.at[m, p], recv_sem=tl_r.at[m, p],
            device_id=above, device_id_type=MESH)

    def base_copy(m):
        return pltpu.make_async_remote_copy(
            src_ref=BASE.at[m], dst_ref=BL.at[m], send_sem=pp_s.at[0, m], recv_sem=pp_r.at[0, m],
            device_id=above, device_id_type=MESH)

    def back_copy(m):
        return pltpu.make_async_remote_copy(
            src_ref=X.at[m], dst_ref=OB.at[m], send_sem=pp_s.at[1, m], recv_sem=pp_r.at[1, m],
            device_id=above, device_id_type=MESH)

    def own_input(m):
        for t in range(n_tok):
            X[m, t : t + 1] = acts[t, m : m + 1]

    def passed_input(m):
        base_copy(m).wait_recv()
        for p in range(3):
            own_copy(m, p).wait_recv()
            tp_copy(m, p, 0).wait_recv()
        X[m] = (BL[m] + (TL[m].astype(F32) + TR[0, m].astype(F32))).astype(BF16)
        back_copy(m).start()

    def norm(m):
        wide = X[m].astype(F32)
        spread = jnp.mean(wide * wide, axis=-1, keepdims=True)
        normed = (wide * lax.rsqrt(spread + 1e-06) * gain[...].astype(F32)).astype(BF16)
        G[m, me[0], me[1], me[2], :, pl.ds(0, width)] = normed
        G[m, me[0], me[1], me[2], :, pl.ds(width, LANES)] = CODE[m].astype(BF16)

    def send(m):
        for p in range(3):
            ag_start(m, p, 0)

    def zero_share(m):
        normed = G[m, me[0], me[1], me[2], :, pl.ds(0, width)]
        gates = jax.nn.sigmoid(dot_t(normed, RT[...]))
        lane = lax.broadcasted_iota(jnp.int32, gates.shape, 1)
        share = jnp.where(lane >= n_real, MASK[m][:, :n_total] * gates, 0.0)
        share = jnp.sum(share, axis=-1, keepdims=True)
        BASE[m] = X[m].astype(F32) + share * normed.astype(F32)

        @pl.when(sec == 0)
        def _():
            base_copy(m).start()

    def tokens(m, start, size):
        return G[m, :, :, :, :, pl.ds(start, size)].reshape(rows, size)

    def work(m):
        mid = rows // 2
        for h in range(2):
            some = G[m, h * (sizes[0] // 2) : (h + 1) * (sizes[0] // 2), :, :, :, pl.ds(0, width)].reshape(mid, width)
            hid = dot_t(some, W1[...])
            LH[h * mid : (h + 1) * mid, 0:LANES] = (jax.nn.silu(hid[:, :LANES]) * hid[:, LANES:]).astype(BF16)
        codes = tokens(m, width, LANES)
        pick = (lax.broadcasted_iota(jnp.int32, (LANES, n_slots), 0) == group).astype(BF16)
        col = jnp.dot(codes, pick, preferred_element_type=F32)
        tok = lax.broadcasted_iota(jnp.int32, (rows, n_slots), 0)
        slot = lax.broadcasted_iota(jnp.int32, (rows, n_slots), 1)
        hit = (tok // ROWS == slot // slots) & (col == (slot % slots + 1).astype(F32))
        LH[:, LANES:] = jnp.where(hit, 1.0, 0.0).astype(BF16)
        pick_t = (lax.broadcasted_iota(jnp.int32, (ROWS, LANES), 1) == group).astype(BF16)
        row = dot_t(pick_t, codes)[0:1]
        slot = lax.broadcasted_iota(jnp.int32, (n_slots, rows), 0)
        tok = lax.broadcasted_iota(jnp.int32, (n_slots, rows), 1)
        hit = (tok // ROWS == slot // slots) & (row == (slot % slots + 1).astype(F32))
        chooser = jnp.where(hit, 1.0, 0.0).astype(BF16)
        if m == 0:
            forward(1)
        for c in range(0, width, chunk):
            CH[:, pl.ds(c, chunk)] = jnp.dot(chooser, tokens(m, c, chunk), preferred_element_type=F32).astype(BF16)
        chosen = CH[...]
        logit = dot_t(chosen, RT[...])
        lane = lax.broadcasted_iota(jnp.int32, logit.shape, 1)
        coef = jax.nn.sigmoid(jnp.sum(jnp.where(lane == group, logit, 0.0), axis=-1, keepdims=True))
        gate = jnp.dot(chosen, EG[...], preferred_element_type=F32)
        up = jnp.dot(chosen, EU[...], preferred_element_type=F32)
        inner = (jax.nn.silu(gate) * up).astype(BF16)
        for c in range(0, width, chunk):
            made = jnp.dot(inner, ED[:, pl.ds(c, chunk)], preferred_element_type=F32)
            DN[pl.ds(LANES, n_slots), pl.ds(c, chunk)] = (coef * made).astype(BF16)

    def put_out(m):
        for p in range(3):
            for c in range(offs[p], offs[p] + part, chunk):
                both = jnp.dot(LH[...], DN[:, pl.ds(c, chunk)], preferred_element_type=F32).astype(BF16)
                PT[m, :, :, :, :, pl.ds(c, chunk)] = both.reshape(*sizes, ROWS, chunk)
            far_start(far_reduce, m, p)

    def rs_sum(m, p, s):
        axis = order[p][2 - s]
        n = sizes[axis]
        if s == 0:
            rest = [d for d in range(3) if d != axis]

            def add(i, carry):
                at = [slice(None)] * 3
                at[axis] = me[axis]
                at[rest[0]] = i
                total = PT[m, at[0], at[1], at[2], :, pl.ds(offs[p], part)].astype(F32)
                for side in range(2):
                    total += RB[m, p, side, i].astype(F32)
                S1[m, p, i] = total.astype(BF16)
                return carry

            lax.fori_loop(0, sizes[rest[0]], add, 0)
        elif s == 1:
            rest = [d for d in range(3) if d != order[p][2]]
            at = [slice(None)] * 2
            at[rest.index(axis)] = me[axis]
            total = S1[m, p, at[0], at[1]].astype(F32)
            for o in range(n - 1):
                total += R2[m, p, o].astype(F32)
            S2[m, p] = total.astype(BF16)
        else:
            total = S2[m, p, me[axis]].astype(F32)
            for o in range(n - 1):
                total += R3[m, p, o].astype(F32)
            TS[m, :, pl.ds(offs[p], part)] = total.astype(BF16)

    def finish(m):
        @pl.when(sec == 0)
        def _():
            back_copy(m).wait_recv()
            for t in range(n_tok):
                out[0, t, m : m + 1] = OB[m, t : t + 1]

        @pl.when(sec == 1)
        def _():
            for p in range(3):
                tp_copy(m, p, 1).wait_recv()
            done = (BASE[m] + (TS[m].astype(F32) + TR[1, m].astype(F32))).astype(BF16)
            for t in range(n_tok):
                out[0, t, m : m + 1] = done[t : t + 1]

    def enter(m):
        passed_input(m)
        norm(m)
        send(m)

    def gather(m, s):
        for p in range(3):
            if s < 2:
                ag_wait(m, p, s)
            else:
                far_wait(far_gather, m, p)
            if s == 0:
                ag_start(m, p, 1)
            elif s == 1:
                far_start(far_gather, m, p)

    def reduce(m, s):
        for p in range(3):
            if s == 0:
                far_wait(far_reduce, m, p)
            else:
                rs_wait(m, p, s)
            rs_sum(m, p, s)
            if s < 2:
                rs_start(m, p, s + 1)
            else:
                tp_copy(m, p, sec).start()

                @pl.when(sec == 0)
                def _():
                    own_copy(m, p).start()

    def sent_gather(m):
        for p in range(3):
            for s in range(2):
                for o in range(1, sizes[order[p][s]]):
                    ag_copy(m, p, s, o).wait_send()
            for k in range(5):
                for way in range(2):
                    far_gather(m, p, way, k).wait_send()

    def sent_reduce(m):
        for p in range(3):
            for s in range(1, 3):
                for o in range(1, sizes[order[p][2 - s]]):
                    rs_copy(m, p, s, o).wait_send()
            for k in range(5):
                for way in range(2):
                    far_reduce(m, p, way, k).wait_send()

    def only(section, *steps):
        @pl.when(sec == section)
        def _():
            for step in steps:
                step()

    only(0, lambda: own_input(0), lambda: norm(0), lambda: own_input(1), lambda: norm(1))
    pl.semaphore_wait(barrier, greeted)
    only(0, lambda: send(0), lambda: send(1))
    only(1, lambda: enter(0))
    gather(0, 0)
    only(1, lambda: enter(1))
    gather(1, 0)
    gather(0, 1)
    forward(0)
    gather(1, 1)
    for c in weight_copies():
        c.wait()
    zero_share(0)
    zero_share(1)
    gather(0, 2)
    work(0)
    put_out(0)
    gather(1, 2)
    work(1)
    merge(0)
    put_out(1)
    merge(1)
    reduce(0, 0)
    reduce(1, 0)
    reduce(0, 1)
    sent_gather(0)
    reduce(1, 1)
    sent_gather(1)
    reduce(0, 2)
    reduce(1, 2)
    sent_reduce(0)
    sent_reduce(1)
    finish(0)
    finish(1)

    for m in range(n_micro):
        for p in range(3):
            tp_copy(m, p, sec).wait_send()

        @pl.when(sec == 0)
        def _():
            for p in range(3):
                own_copy(m, p).wait_send()
            base_copy(m).wait_send()

        @pl.when(sec == 1)
        def _():
            back_copy(m).wait_send()


def on_device(sizes, n_tp, acts, routes, gain, router, dg, du, dd, eg, eu, ed):
    swapped = (jnp.swapaxes(acts, 0, 1), jnp.swapaxes(routes, 1, 2), gain, *(jnp.swapaxes(w, 1, 2) for w in (router, dg, du)))
    return jnp.swapaxes(in_vmem(sizes, n_tp, *swapped, dd, eg, eu, ed), 1, 2)


def in_vmem(sizes, n_tp, acts, routes, gain, router, dg, du, dd, eg, eu, ed):
    n_tok, n_micro, width = acts.shape
    topk = routes.shape[-1]
    n_total = router.shape[1]
    n_blocks = sizes[0] * sizes[1] * sizes[2]
    slots = max(2, (n_tok * topk + n_total - 1) // n_total)
    n_slots = n_blocks * slots
    part = width // 3
    chunk = min(512, part)
    n = sizes[0]
    inner = eg.shape[-1]
    cfg = (sizes, n_tp, width, n_micro, n_tok, topk, n_blocks, n_total, slots, chunk)
    vm = pltpu.VMEM
    scratch = [
        vm((n_micro, *sizes, ROWS, width + LANES), BF16),
        vm((n_micro, *sizes, ROWS, width), BF16),
        vm((n_micro, 3, 2, n, n, ROWS, part // 2), BF16),
        vm((n_micro, 3, 2, n, n, ROWS, part), BF16),
        vm((n_micro, 3, n, n, ROWS, part), BF16),
        vm((n_micro, 3, n - 1, n, ROWS, part), BF16),
        vm((n_micro, 3, n, ROWS, part), BF16),
        vm((n_micro, 3, n - 1, ROWS, part), BF16),
        vm((n_micro, ROWS, width), BF16),
        vm((2, n_micro, ROWS, width), BF16),
        vm((n_micro, ROWS, width), BF16),
        vm((n_micro, ROWS, width), F32),
        vm((n_micro, ROWS, width), F32),
        vm((n_micro, ROWS, width), BF16),
        vm((n_micro, ROWS, width), BF16),
        vm((n_micro, ROWS, LANES), F32),
        vm((n_micro, ROWS, LANES), F32),
        vm((n_total, width), BF16),
        vm((width, inner), BF16),
        vm((width, inner), BF16),
        vm((inner, width), BF16),
        vm((2 * LANES, width), BF16),
        vm((n_blocks * ROWS, LANES + n_slots), BF16),
        vm((LANES + n_slots, width), BF16),
        vm((n_slots, width), BF16),
        pltpu.SemaphoreType.DMA((7,)),
        pltpu.SemaphoreType.DMA((n_micro, 3, 2, n - 1)),
        pltpu.SemaphoreType.DMA((n_micro, 3, 2, n - 1)),
        pltpu.SemaphoreType.DMA((n_micro, 3, 2, n - 1)),
        pltpu.SemaphoreType.DMA((n_micro, 3, 2, n - 1)),
        pltpu.SemaphoreType.DMA((n_micro, 3, 2, 5)),
        pltpu.SemaphoreType.DMA((n_micro, 3, 2, 5)),
        pltpu.SemaphoreType.DMA((n_micro, 3, 2, 5)),
        pltpu.SemaphoreType.DMA((n_micro, 3, 2, 5)),
        pltpu.SemaphoreType.DMA((n_micro, 3)),
        pltpu.SemaphoreType.DMA((2, n_micro, 3)),
        pltpu.SemaphoreType.DMA((n_micro, 3)),
        pltpu.SemaphoreType.DMA((n_micro, 3)),
        pltpu.SemaphoreType.DMA((2, n_micro)),
        pltpu.SemaphoreType.DMA((2, n_micro)),
    ]
    held = pl.BlockSpec(memory_space=pltpu.VMEM)
    left = pl.BlockSpec(memory_space=pltpu.HBM)
    return pl.pallas_call(
        functools.partial(kernel, cfg),
        out_shape=jax.ShapeDtypeStruct((1, n_tok, n_micro, width), BF16),
        in_specs=[held] * 3 + [left] * 7,
        out_specs=held,
        scratch_shapes=scratch,
        compiler_params=pltpu.CompilerParams(
            collective_id=0, has_side_effects=True, vmem_limit_bytes=60 * 1024 * 1024
        ),
        name="relay",
    )(acts, routes, gain, router, dg, du, dd, eg, eu, ed)


def solution(mesh):
    n_tp = mesh.shape["tp"]
    side = round(mesh.shape["ep"] ** (1 / 3))
    sizes = (side, side, side)
    finer = Mesh(
        mesh.devices.reshape(mesh.shape["pp"], *sizes, n_tp),
        ("pp", "ep_0", "ep_1", "ep_2", "tp"),
    )
    in_specs = (
        P(None, EP, None),
        P("pp", None, EP, None),
        P("pp", None),
        P("pp", None, None),
        P("pp", None, EP_TP),
        P("pp", None, EP_TP),
        P("pp", EP_TP, None),
        P("pp", EP, None, "tp"),
        P("pp", EP, None, "tp"),
        P("pp", EP, "tp", None),
    )
    return jax.shard_map(
        functools.partial(on_device, sizes, n_tp),
        mesh=finer,
        in_specs=in_specs,
        out_specs=P("pp", None, EP, None),
        check_vma=False,
    )
```

```python
import functools

import jax
import jax.numpy as jnp
from jax import lax
from jax.experimental import pallas as pl
from jax.experimental.pallas import tpu as pltpu
from jax.sharding import Mesh
from jax.sharding import PartitionSpec as P

MESH = pl.DeviceIdType.MESH
EP = ("ep_0", "ep_1", "ep_2")
EP_TP = ("ep_0", "ep_1", "ep_2", "tp")
F32 = jnp.float32
BF16 = jnp.bfloat16
ROWS = 8
LANES = 128


def farthest_first(n):
    return sorted(range(1, n), key=lambda o: -min(o, n - o))


def dot_t(a, b):
    return lax.dot_general(a, b, (((1,), (1,)), ((), ())), preferred_element_type=F32)


def kernel(cfg, *refs):
    (acts, routes, gain, router_h, dg_h, du_h, dd_h, eg_h, eu_h, ed_h, out) = refs[:11]
    (G, PT, RA, RB, S1, R2, S2, R3, TS, TR, TL, BASE, BL, X, OB, CODE, MASK) = refs[11:28]
    (RT, EG, EU, ED, W1, LH, DN, CH) = refs[28:36]
    (w_sem, ag_s, ag_r, rs_s, rs_r, fa_s, fa_r, fr_s, fr_r, tp_s, tp_r, tl_s, tl_r, pp_s, pp_r) = refs[36:]
    sizes, n_tp, width, n_micro, n_tok, topk, n_real, n_total, slots, chunk = cfg
    n_blocks = sizes[0] * sizes[1] * sizes[2]
    rows = n_blocks * ROWS
    n_slots = n_blocks * slots
    part = width // 3
    offs = (0, part, 2 * part)
    gw = (part, part, part + LANES)
    order = ((0, 1, 2), (1, 2, 0), (2, 0, 1))

    sec = lax.axis_index("pp")
    me = tuple(lax.axis_index(a) for a in EP)
    tp = lax.axis_index("tp")
    group = (me[0] * sizes[1] + me[1]) * sizes[2] + me[2]

    def peer(axis, o):
        n = sizes[axis]
        if axis != 1:
            return {EP[axis]: lax.rem(me[axis] + o + n, n)}
        step = o if abs(o) <= n // 2 else o - n * (o // abs(o))
        z = lax.rem(tp * n + me[1] + step + n * n_tp, n * n_tp)
        return {"ep_1": lax.rem(z, n), "tp": z // n}

    far_last = {"tp": 1 - tp, "pp": 1}
    above = {"pp": 1 - sec}

    def weight_copies():
        hidden = dg_h.shape[1]
        pairs = ((router_h.at[0], RT), (dg_h.at[0], W1.at[pl.ds(0, hidden)]), (du_h.at[0], W1.at[pl.ds(LANES, hidden)]),
                 (dd_h.at[0], DN.at[pl.ds(0, hidden)]),
                 (eg_h.at[0, 0], EG), (eu_h.at[0, 0], EU), (ed_h.at[0, 0], ED))
        return [pltpu.make_async_copy(s, d, w_sem.at[i]) for i, (s, d) in enumerate(pairs)]

    for c in weight_copies():
        c.start()

    X[...] = jnp.zeros_like(X)
    barrier = pltpu.get_barrier_semaphore()
    greeted = 0
    for axis in range(3):
        for o in range(1, sizes[axis]):
            pl.semaphore_signal(barrier, inc=1, device_id=peer(axis, -o), device_id_type=MESH)
            greeted += 1
    pl.semaphore_signal(barrier, inc=1, device_id=above, device_id_type=MESH)
    greeted += 1

    CODE[...] = jnp.zeros_like(CODE)
    MASK[...] = jnp.zeros_like(MASK)
    spare = LANES - dd_h.shape[1]
    for ref, start in ((W1, LANES - spare), (W1, 2 * LANES - spare), (DN, LANES - spare)):
        ref[pl.ds(start, spare)] = jnp.zeros((spare, width), BF16)
    for m in range(n_micro):
        ids = jnp.concatenate([routes[0, t, m : m + 1] for t in range(n_tok)], axis=0)
        lane = lax.broadcasted_iota(jnp.int32, (n_tok, LANES), 1)
        named = jnp.zeros((n_tok, LANES), F32)
        for k in range(topk):
            named += (ids[:, k : k + 1] == lane).astype(F32)
        MASK[m, 0:n_tok] = named
        before = jnp.zeros((1, LANES), F32)
        for t in range(n_tok):
            row = named[t : t + 1]
            CODE[m, t : t + 1] = row * (before + 1.0)
            before += row

    def ag_copy(m, p, s, o):
        axes = order[p]
        at = [me[0], me[1], me[2]]
        for a in axes[:s]:
            at[a] = slice(None)
        ref = G.at[m, at[0], at[1], at[2], :, pl.ds(offs[p], gw[p])]
        return pltpu.make_async_remote_copy(
            src_ref=ref, dst_ref=ref, send_sem=ag_s.at[m, p, s, o - 1], recv_sem=ag_r.at[m, p, s, o - 1],
            device_id=peer(axes[s], o), device_id_type=MESH)

    def ag_start(m, p, s):
        for o in farthest_first(sizes[order[p][s]]):
            ag_copy(m, p, s, o).start()

    def ag_wait(m, p, s):
        for o in range(1, sizes[order[p][s]]):
            ag_copy(m, p, s, o).wait_recv()

    def rs_refs(m, p, s, o):
        axis = order[p][2 - s]
        there = lax.rem(me[axis] + o, sizes[axis])
        if s == 1:
            rest = [d for d in range(3) if d != order[p][2]]
            at = [slice(None)] * 2
            at[rest.index(axis)] = there
            return S1.at[m, p, at[0], at[1]], R2.at[m, p, o - 1]
        return S2.at[m, p, there], R3.at[m, p, o - 1]

    def rs_copy(m, p, s, o):
        src, dst = rs_refs(m, p, s, o)
        return pltpu.make_async_remote_copy(
            src_ref=src, dst_ref=dst, send_sem=rs_s.at[m, p, s - 1, o - 1], recv_sem=rs_r.at[m, p, s - 1, o - 1],
            device_id=peer(order[p][2 - s], o), device_id_type=MESH)

    def rs_start(m, p, s):
        for o in farthest_first(sizes[order[p][2 - s]]):
            rs_copy(m, p, s, o).start()

    def rs_wait(m, p, s):
        for o in range(1, sizes[order[p][2 - s]]):
            rs_copy(m, p, s, o).wait_recv()

    def plane(ref, m, axis, there, start, size):
        at = [slice(None)] * 3
        at[axis] = there
        return ref.at[m, at[0], at[1], at[2], :, pl.ds(start, size)]

    half, quarter = part // 2, part // 4

    def lanes_of(p, way, k, width_p):
        if k == 2:
            return ((1 - way) * half, half if way == 1 else width_p - half)
        start = way * half + (k % 3) * quarter
        return (start, width_p - start if way == 1 and k % 3 == 1 else quarter)

    def far_gather(m, p, way, k):
        axis = order[p][2]
        shift = 0 if k < 3 else (-1, 1)[way]
        start, size = lanes_of(p, way, k, gw[p])
        ref = plane(G, m, axis, lax.rem(me[axis] + sizes[axis] + shift, sizes[axis]), offs[p] + start, size)
        return pltpu.make_async_remote_copy(
            src_ref=ref, dst_ref=ref, send_sem=fa_s.at[m, p, way, k], recv_sem=fa_r.at[m, p, way, k],
            device_id=peer(axis, (1, -1)[way]), device_id_type=MESH)

    def far_reduce(m, p, way, k):
        axis = order[p][2]
        n = sizes[axis]
        start, size = lanes_of(p, way, k, part)
        src = plane(PT, m, axis, lax.rem(me[axis] + (2 if k < 2 else (1, n - 1)[way]), n), offs[p] + start, size)
        if k < 2:
            dst = RA.at[m, p, way, :, :, :, pl.ds(k * quarter, quarter)]
        else:
            dst = RB.at[m, p, way, :, :, :, pl.ds(start, size)]
        return pltpu.make_async_remote_copy(
            src_ref=src, dst_ref=dst, send_sem=fr_s.at[m, p, way, k], recv_sem=fr_r.at[m, p, way, k],
            device_id=peer(axis, (1, -1)[way]), device_id_type=MESH)

    def far_start(copy, m, p):
        for k in range(3):
            for way in range(2):
                copy(m, p, way, k).start()

    def far_wait(copy, m, p):
        for k in range(2, 5):
            for way in range(2):
                copy(m, p, way, k).wait_recv()

    def forward(m):
        for k in range(2):
            for p in range(3):
                for way in range(2):
                    far_gather(m, p, way, k).wait_recv()
                    far_gather(m, p, way, k + 3).start()

    def merge(m):
        for k in range(2):
            for p in range(3):
                axis = order[p][2]
                rest = [d for d in range(3) if d != axis]
                for way in range(2):
                    far_reduce(m, p, way, k).wait_recv()
                    at = [slice(None)] * 3
                    at[axis] = lax.rem(me[axis] + (1, sizes[axis] - 1)[way], sizes[axis])
                    where = (m, *at, slice(None), pl.ds(offs[p] + way * half + k * quarter, quarter))
                    PT[where] = PT[where] + RA[m, p, way, :, :, :, pl.ds(k * quarter, quarter)]
                    far_reduce(m, p, way, k + 3).start()

    def tp_copy(m, p, section):
        lanes = pl.ds(offs[p], part)
        return pltpu.make_async_remote_copy(
            src_ref=TS.at[m, :, lanes], dst_ref=TR.at[section, m, :, lanes], send_sem=tp_s.at[m, p],
            recv_sem=tp_r.at[section, m, p], device_id=far_last, device_id_type=MESH)

    def own_copy(m, p):
        lanes = pl.ds(offs[p], part)
        return pltpu.make_async_remote_copy(
            src_ref=TS.at[m, :, lanes], dst_ref=TL.at[m, :, lanes], send_sem=tl_s.at[m, p], recv_sem=tl_r.at[m, p],
            device_id=above, device_id_type=MESH)

    def base_copy(m):
        return pltpu.make_async_remote_copy(
            src_ref=BASE.at[m], dst_ref=BL.at[m], send_sem=pp_s.at[0, m], recv_sem=pp_r.at[0, m],
            device_id=above, device_id_type=MESH)

    def back_copy(m):
        return pltpu.make_async_remote_copy(
            src_ref=X.at[m], dst_ref=OB.at[m], send_sem=pp_s.at[1, m], recv_sem=pp_r.at[1, m],
            device_id=above, device_id_type=MESH)

    def own_input(m):
        for t in range(n_tok):
            X[m, t : t + 1] = acts[t, m : m + 1]

    def passed_input(m):
        base_copy(m).wait_recv()
        for p in range(3):
            own_copy(m, p).wait_recv()
            tp_copy(m, p, 0).wait_recv()
        X[m] = (BL[m] + (TL[m].astype(F32) + TR[0, m].astype(F32))).astype(BF16)
        back_copy(m).start()

    def norm(m):
        wide = X[m].astype(F32)
        spread = jnp.mean(wide * wide, axis=-1, keepdims=True)
        normed = (wide * lax.rsqrt(spread + 1e-06) * gain[...].astype(F32)).astype(BF16)
        G[m, me[0], me[1], me[2], :, pl.ds(0, width)] = normed
        G[m, me[0], me[1], me[2], :, pl.ds(width, LANES)] = CODE[m].astype(BF16)

    def send(m):
        for p in range(3):
            ag_start(m, p, 0)

    def zero_share(m):
        normed = G[m, me[0], me[1], me[2], :, pl.ds(0, width)]
        gates = jax.nn.sigmoid(dot_t(normed, RT[...]))
        lane = lax.broadcasted_iota(jnp.int32, gates.shape, 1)
        share = jnp.where(lane >= n_real, MASK[m][:, :n_total] * gates, 0.0)
        share = jnp.sum(share, axis=-1, keepdims=True)
        BASE[m] = X[m].astype(F32) + share * normed.astype(F32)

        @pl.when(sec == 0)
        def _():
            base_copy(m).start()

    def tokens(m, start, size):
        return G[m, :, :, :, :, pl.ds(start, size)].reshape(rows, size)

    def work(m):
        mid = rows // 2
        for h in range(2):
            some = G[m, h * (sizes[0] // 2) : (h + 1) * (sizes[0] // 2), :, :, :, pl.ds(0, width)].reshape(mid, width)
            hid = dot_t(some, W1[...])
            LH[h * mid : (h + 1) * mid, 0:LANES] = (jax.nn.silu(hid[:, :LANES]) * hid[:, LANES:]).astype(BF16)
        codes = tokens(m, width, LANES)
        pick = (lax.broadcasted_iota(jnp.int32, (LANES, n_slots), 0) == group).astype(BF16)
        col = jnp.dot(codes, pick, preferred_element_type=F32)
        tok = lax.broadcasted_iota(jnp.int32, (rows, n_slots), 0)
        slot = lax.broadcasted_iota(jnp.int32, (rows, n_slots), 1)
        hit = (tok // ROWS == slot // slots) & (col == (slot % slots + 1).astype(F32))
        LH[:, LANES:] = jnp.where(hit, 1.0, 0.0).astype(BF16)
        pick_t = (lax.broadcasted_iota(jnp.int32, (ROWS, LANES), 1) == group).astype(BF16)
        row = dot_t(pick_t, codes)[0:1]
        slot = lax.broadcasted_iota(jnp.int32, (n_slots, rows), 0)
        tok = lax.broadcasted_iota(jnp.int32, (n_slots, rows), 1)
        hit = (tok // ROWS == slot // slots) & (row == (slot % slots + 1).astype(F32))
        chooser = jnp.where(hit, 1.0, 0.0).astype(BF16)
        if m == 0:
            forward(1)
        for c in range(0, width, chunk):
            CH[:, pl.ds(c, chunk)] = jnp.dot(chooser, tokens(m, c, chunk), preferred_element_type=F32).astype(BF16)
        chosen = CH[...]
        logit = dot_t(chosen, RT[...])
        lane = lax.broadcasted_iota(jnp.int32, logit.shape, 1)
        coef = jax.nn.sigmoid(jnp.sum(jnp.where(lane == group, logit, 0.0), axis=-1, keepdims=True))
        gate = jnp.dot(chosen, EG[...], preferred_element_type=F32)
        up = jnp.dot(chosen, EU[...], preferred_element_type=F32)
        inner = (jax.nn.silu(gate) * up).astype(BF16)
        for c in range(0, width, chunk):
            made = jnp.dot(inner, ED[:, pl.ds(c, chunk)], preferred_element_type=F32)
            DN[pl.ds(LANES, n_slots), pl.ds(c, chunk)] = (coef * made).astype(BF16)

    def put_out(m):
        for p in range(3):
            for c in range(offs[p], offs[p] + part, chunk):
                both = jnp.dot(LH[...], DN[:, pl.ds(c, chunk)], preferred_element_type=F32).astype(BF16)
                PT[m, :, :, :, :, pl.ds(c, chunk)] = both.reshape(*sizes, ROWS, chunk)
            far_start(far_reduce, m, p)

    def rs_sum(m, p, s):
        axis = order[p][2 - s]
        n = sizes[axis]
        if s == 0:
            rest = [d for d in range(3) if d != axis]

            def add(i, carry):
                at = [slice(None)] * 3
                at[axis] = me[axis]
                at[rest[0]] = i
                total = PT[m, at[0], at[1], at[2], :, pl.ds(offs[p], part)].astype(F32)
                for side in range(2):
                    total += RB[m, p, side, i].astype(F32)
                S1[m, p, i] = total.astype(BF16)
                return carry

            lax.fori_loop(0, sizes[rest[0]], add, 0)
        elif s == 1:
            rest = [d for d in range(3) if d != order[p][2]]
            at = [slice(None)] * 2
            at[rest.index(axis)] = me[axis]
            total = S1[m, p, at[0], at[1]].astype(F32)
            for o in range(n - 1):
                total += R2[m, p, o].astype(F32)
            S2[m, p] = total.astype(BF16)
        else:
            total = S2[m, p, me[axis]].astype(F32)
            for o in range(n - 1):
                total += R3[m, p, o].astype(F32)
            TS[m, :, pl.ds(offs[p], part)] = total.astype(BF16)

    def finish(m):
        @pl.when(sec == 0)
        def _():
            back_copy(m).wait_recv()
            for t in range(n_tok):
                out[0, t, m : m + 1] = OB[m, t : t + 1]

        @pl.when(sec == 1)
        def _():
            for p in range(3):
                tp_copy(m, p, 1).wait_recv()
            done = (BASE[m] + (TS[m].astype(F32) + TR[1, m].astype(F32))).astype(BF16)
            for t in range(n_tok):
                out[0, t, m : m + 1] = done[t : t + 1]

    def enter(m):
        passed_input(m)
        norm(m)
        send(m)

    def gather(m, s):
        for p in range(3):
            if s < 2:
                ag_wait(m, p, s)
            else:
                far_wait(far_gather, m, p)
            if s == 0:
                ag_start(m, p, 1)
            elif s == 1:
                far_start(far_gather, m, p)

    def reduce(m, s):
        for p in range(3):
            if s == 0:
                far_wait(far_reduce, m, p)
            else:
                rs_wait(m, p, s)
            rs_sum(m, p, s)
            if s < 2:
                rs_start(m, p, s + 1)
            else:
                tp_copy(m, p, sec).start()

                @pl.when(sec == 0)
                def _():
                    own_copy(m, p).start()

    def sent_gather(m):
        for p in range(3):
            for s in range(2):
                for o in range(1, sizes[order[p][s]]):
                    ag_copy(m, p, s, o).wait_send()
            for k in range(5):
                for way in range(2):
                    far_gather(m, p, way, k).wait_send()

    def sent_reduce(m):
        for p in range(3):
            for s in range(1, 3):
                for o in range(1, sizes[order[p][2 - s]]):
                    rs_copy(m, p, s, o).wait_send()
            for k in range(5):
                for way in range(2):
                    far_reduce(m, p, way, k).wait_send()

    def only(section, *steps):
        @pl.when(sec == section)
        def _():
            for step in steps:
                step()

    only(0, lambda: own_input(0), lambda: norm(0), lambda: own_input(1), lambda: norm(1))
    pl.semaphore_wait(barrier, greeted)
    only(0, lambda: send(0), lambda: send(1))
    only(1, lambda: enter(0))
    gather(0, 0)
    only(1, lambda: enter(1))
    gather(1, 0)
    gather(0, 1)
    forward(0)
    gather(1, 1)
    for c in weight_copies():
        c.wait()
    zero_share(0)
    zero_share(1)
    gather(0, 2)
    work(0)
    put_out(0)
    gather(1, 2)
    work(1)
    merge(0)
    put_out(1)
    merge(1)
    reduce(0, 0)
    reduce(1, 0)
    reduce(0, 1)
    sent_gather(0)
    reduce(1, 1)
    sent_gather(1)
    reduce(0, 2)
    reduce(1, 2)
    sent_reduce(0)
    sent_reduce(1)
    finish(0)
    finish(1)

    for m in range(n_micro):
        for p in range(3):
            tp_copy(m, p, sec).wait_send()

        @pl.when(sec == 0)
        def _():
            for p in range(3):
                own_copy(m, p).wait_send()
            base_copy(m).wait_send()

        @pl.when(sec == 1)
        def _():
            back_copy(m).wait_send()


def on_device(sizes, n_tp, acts, routes, gain, router, dg, du, dd, eg, eu, ed):
    swapped = (jnp.swapaxes(acts, 0, 1), jnp.swapaxes(routes, 1, 2), gain, *(jnp.swapaxes(w, 1, 2) for w in (router, dg, du)))
    return jnp.swapaxes(in_vmem(sizes, n_tp, *swapped, dd, eg, eu, ed), 1, 2)


def in_vmem(sizes, n_tp, acts, routes, gain, router, dg, du, dd, eg, eu, ed):
    n_tok, n_micro, width = acts.shape
    topk = routes.shape[-1]
    n_total = router.shape[1]
    n_blocks = sizes[0] * sizes[1] * sizes[2]
    slots = max(2, (n_tok * topk + n_total - 1) // n_total)
    n_slots = n_blocks * slots
    part = width // 3
    chunk = min(512, part)
    n = sizes[0]
    inner = eg.shape[-1]
    cfg = (sizes, n_tp, width, n_micro, n_tok, topk, n_blocks, n_total, slots, chunk)
    vm = pltpu.VMEM
    scratch = [
        vm((n_micro, *sizes, ROWS, width + LANES), BF16),
        vm((n_micro, *sizes, ROWS, width), BF16),
        vm((n_micro, 3, 2, n, n, ROWS, part // 2), BF16),
        vm((n_micro, 3, 2, n, n, ROWS, part), BF16),
        vm((n_micro, 3, n, n, ROWS, part), BF16),
        vm((n_micro, 3, n - 1, n, ROWS, part), BF16),
        vm((n_micro, 3, n, ROWS, part), BF16),
        vm((n_micro, 3, n - 1, ROWS, part), BF16),
        vm((n_micro, ROWS, width), BF16),
        vm((2, n_micro, ROWS, width), BF16),
        vm((n_micro, ROWS, width), BF16),
        vm((n_micro, ROWS, width), F32),
        vm((n_micro, ROWS, width), F32),
        vm((n_micro, ROWS, width), BF16),
        vm((n_micro, ROWS, width), BF16),
        vm((n_micro, ROWS, LANES), F32),
        vm((n_micro, ROWS, LANES), F32),
        vm((n_total, width), BF16),
        vm((width, inner), BF16),
        vm((width, inner), BF16),
        vm((inner, width), BF16),
        vm((2 * LANES, width), BF16),
        vm((n_blocks * ROWS, LANES + n_slots), BF16),
        vm((LANES + n_slots, width), BF16),
        vm((n_slots, width), BF16),
        pltpu.SemaphoreType.DMA((7,)),
        pltpu.SemaphoreType.DMA((n_micro, 3, 2, n - 1)),
        pltpu.SemaphoreType.DMA((n_micro, 3, 2, n - 1)),
        pltpu.SemaphoreType.DMA((n_micro, 3, 2, n - 1)),
        pltpu.SemaphoreType.DMA((n_micro, 3, 2, n - 1)),
        pltpu.SemaphoreType.DMA((n_micro, 3, 2, 5)),
        pltpu.SemaphoreType.DMA((n_micro, 3, 2, 5)),
        pltpu.SemaphoreType.DMA((n_micro, 3, 2, 5)),
        pltpu.SemaphoreType.DMA((n_micro, 3, 2, 5)),
        pltpu.SemaphoreType.DMA((n_micro, 3)),
        pltpu.SemaphoreType.DMA((2, n_micro, 3)),
        pltpu.SemaphoreType.DMA((n_micro, 3)),
        pltpu.SemaphoreType.DMA((n_micro, 3)),
        pltpu.SemaphoreType.DMA((2, n_micro)),
        pltpu.SemaphoreType.DMA((2, n_micro)),
    ]
    held = pl.BlockSpec(memory_space=pltpu.VMEM)
    left = pl.BlockSpec(memory_space=pltpu.HBM)
    return pl.pallas_call(
        functools.partial(kernel, cfg),
        out_shape=jax.ShapeDtypeStruct((1, n_tok, n_micro, width), BF16),
        in_specs=[held] * 3 + [left] * 7,
        out_specs=held,
        scratch_shapes=scratch,
        compiler_params=pltpu.CompilerParams(
            collective_id=0, has_side_effects=True, vmem_limit_bytes=60 * 1024 * 1024
        ),
        name="relay",
    )(acts, routes, gain, router, dg, du, dd, eg, eu, ed)


def solution(mesh):
    n_tp = mesh.shape["tp"]
    side = round(mesh.shape["ep"] ** (1 / 3))
    sizes = (side, side, side)
    finer = Mesh(
        mesh.devices.reshape(mesh.shape["pp"], *sizes, n_tp),
        ("pp", "ep_0", "ep_1", "ep_2", "tp"),
    )
    in_specs = (
        P(None, EP, None),
        P("pp", None, EP, None),
        P("pp", None),
        P("pp", None, None),
        P("pp", None, EP_TP),
        P("pp", None, EP_TP),
        P("pp", EP_TP, None),
        P("pp", EP, None, "tp"),
        P("pp", EP, None, "tp"),
        P("pp", EP, "tp", None),
    )
    return jax.shard_map(
        functools.partial(on_device, sizes, n_tp),
        mesh=finer,
        in_specs=in_specs,
        out_specs=P("pp", None, EP, None),
        check_vma=False,
    )
```
